16 devices in a mesh: dp: 16 (over z, y, x, core).
Axes of the slice: x: 2, y: 2, z: 2, core: 2. Of those that a mesh axis runs over, the one named last changes fastest.
Arguments:
- query: bfloat16 [512, 28, 128], P('dp')
- k_cache: bfloat16 [512, 512, 4, 128], P('dp')
- v_cache: bfloat16 [512, 512, 4, 128], P('dp')
- cache_lens: int32 [512], P('dp')
- dest_slot: int32 [512], replicated
- k_new: bfloat16 [512, 4, 128], P('dp')
- v_new: bfloat16 [512, 4, 128], P('dp')
Outputs:
- output 1: bfloat16 [512, 28, 128], P('dp')
- output 2: bfloat16 [512, 512, 4, 128], P('dp')
- output 3: bfloat16 [512, 512, 4, 128], P('dp')
- output 4: int32 [512], P('dp')
All inputs are finite; a program needn't handle non-finite values.
Results may differ from the reference program's by a relative error of at most 0.001.
Values are sent between devices in bfloat16 or wider.
A program may use at most 1 GiB of HBM per device.

```python
import jax
import jax.numpy as jnp
from jax import lax

Q_HEADS = 28
KV_HEADS = 4
HEAD_DIM = 128
CACHE_LEN = 512
SLOTS_DEV = 32
GROUP_SIZE = 16
TOTAL_SLOTS = GROUP_SIZE * SLOTS_DEV


def draw_plan(key):
    key_heavy, key_len, key_coin, key_perm = jax.random.split(key, 4)
    heavy_dev = jax.random.randint(key_heavy, (GROUP_SIZE,), 0, 2, dtype=jnp.int32)
    heavy_dev = heavy_dev.at[0].set(1).at[GROUP_SIZE - 1].set(0)
    heavy_slot = jnp.repeat(heavy_dev, SLOTS_DEV)
    len_low = jnp.where(heavy_slot == 1, CACHE_LEN // 2, CACHE_LEN // 16).astype(jnp.int32)
    len_high = jnp.where(heavy_slot == 1, CACHE_LEN, CACHE_LEN // 2).astype(jnp.int32)
    cache_lens = jax.random.randint(key_len, (TOTAL_SLOTS,), len_low, len_high, dtype=jnp.int32)
    cache_lens = cache_lens.at[0].set(CACHE_LEN - 1).at[TOTAL_SLOTS - 1].set(CACHE_LEN // 16)
    move_coin = jax.random.randint(key_coin, (TOTAL_SLOTS,), 0, 4, dtype=jnp.int32)
    moving = (heavy_slot == 1) | (move_coin == 0)
    moving = moving.at[TOTAL_SLOTS - 1].set(True)
    rand_rank = jax.random.permutation(key_perm, TOTAL_SLOTS).astype(jnp.int32)
    sort_score = jnp.where(moving, 0, TOTAL_SLOTS).astype(jnp.int32) + rand_rank
    slot_order = jnp.argsort(sort_score).astype(jnp.int32)
    move_count = jnp.sum(moving.astype(jnp.int32))
    slot_ids = jnp.arange(TOTAL_SLOTS, dtype=jnp.int32)
    next_pos = jnp.where(slot_ids < move_count, (slot_ids + 1) % jnp.maximum(move_count, 1), slot_ids)
    dest_slot = jnp.zeros((TOTAL_SLOTS,), jnp.int32).at[slot_order].set(slot_order[next_pos])
    return cache_lens, dest_slot


def setup_inputs(seed: int = 0) -> dict:
    key = jax.random.key(seed)
    key_plan, key_query, key_kcache, key_vcache, key_knew, key_vnew = jax.random.split(key, 6)
    cache_lens, dest_slot = draw_plan(key_plan)
    query = jax.random.normal(key_query, (TOTAL_SLOTS, Q_HEADS, HEAD_DIM), jnp.float32).astype(jnp.bfloat16)
    k_cache = jax.random.normal(key_kcache, (TOTAL_SLOTS, CACHE_LEN, KV_HEADS, HEAD_DIM), jnp.float32).astype(jnp.bfloat16)
    v_cache = jax.random.normal(key_vcache, (TOTAL_SLOTS, CACHE_LEN, KV_HEADS, HEAD_DIM), jnp.float32).astype(jnp.bfloat16)
    k_new = jax.random.normal(key_knew, (TOTAL_SLOTS, KV_HEADS, HEAD_DIM), jnp.float32).astype(jnp.bfloat16)
    v_new = jax.random.normal(key_vnew, (TOTAL_SLOTS, KV_HEADS, HEAD_DIM), jnp.float32).astype(jnp.bfloat16)
    return {'query': query, 'k_cache': k_cache, 'v_cache': v_cache, 'cache_lens': cache_lens, 'dest_slot': dest_slot, 'k_new': k_new, 'v_new': v_new}


def attend_one(slot_data):
    query_row, k_row, v_row, length = slot_data
    groups = Q_HEADS // KV_HEADS
    q_grp = query_row.reshape(KV_HEADS, groups, HEAD_DIM).astype(jnp.float32)
    scores = jnp.einsum('kgd,tkd->kgt', q_grp, k_row.astype(jnp.float32)) * (HEAD_DIM ** -0.5)
    positions = jnp.arange(CACHE_LEN, dtype=jnp.int32)
    scores = jnp.where((positions <= length)[None, None, :], scores, -1e30)
    score_max = jnp.max(scores, axis=-1, keepdims=True)
    weights = jnp.exp(scores - score_max)
    prob_sum = jnp.sum(weights, axis=-1, keepdims=True)
    probs = weights.astype(jnp.bfloat16).astype(jnp.float32)
    attn_acc = jnp.einsum('kgt,tkd->kgd', probs, v_row.astype(jnp.float32)) / prob_sum
    return attn_acc.astype(jnp.bfloat16).reshape(Q_HEADS, HEAD_DIM)


def reference(query, k_cache, v_cache, cache_lens, dest_slot, k_new, v_new):
    slot_ids = jnp.arange(TOTAL_SLOTS, dtype=jnp.int32)
    source = jnp.zeros((TOTAL_SLOTS,), jnp.int32).at[dest_slot].set(slot_ids)
    lens_new = cache_lens[source]
    positions = jnp.arange(CACHE_LEN, dtype=jnp.int32)
    keep_row = (positions[None, :] < lens_new[:, None])[:, :, None, None]
    at_new = (positions[None, :] == lens_new[:, None])[:, :, None, None]
    zero_val = jnp.zeros((), jnp.bfloat16)
    k_out = jnp.where(keep_row, k_cache[source], jnp.where(at_new, k_new[:, None], zero_val))
    v_out = jnp.where(keep_row, v_cache[source], jnp.where(at_new, v_new[:, None], zero_val))
    attn_out = lax.map(attend_one, (query, k_out, v_out, lens_new))
    return attn_out, k_out, v_out, lens_new + 1
```

```python
import functools
import itertools

import jax
import jax.numpy as jnp
import numpy as np
from jax import lax
from jax.experimental import pallas as pl
from jax.experimental.pallas import tpu as pltpu
from jax.sharding import PartitionSpec as P

I32, F32, BF = jnp.int32, jnp.float32, jnp.bfloat16
DEVS, SLOTS, TOTAL = 16, 32, 512
CHIPS, CHIP_SLOTS = 8, 64
ROWS = 512
HEADS, KV, DIM, GROUP = 28, 4, 128, 7
LANES = 128
HALF = 8192
CLASSES = ((1152, 6144), (1312, 6144), (1472, 6144), (1632, 6144), (1824, 6144), (2048, 6144), (2400, HALF))
ITERS = 12
LAST = jnp.iinfo(jnp.int32).max
VMEM_LIMIT = 60 * 1024 * 1024


def make_options():
    found = []
    for b in range(1, 8):
        dims = [k for k in range(3) if (b >> k) & 1]
        mine = []
        for steps in itertools.combinations(range(3), len(dims)):
            for order in itertools.permutations(dims):
                place, hops = 0, []
                for step, k in zip(steps, order):
                    hops.append((step, place, k))
                    place ^= 1 << k
                mine.append((b, tuple(hops)))
        mine.sort(key=lambda option: (option[1][0][0], option[1][0][2], option[1]))
        found += mine
    return found


OPTIONS = make_options()
N_OPT = len(OPTIONS)
OPT_BASE = [next(o for o in range(N_OPT) if OPTIONS[o][0] == b) for b in range(1, 8)]
OPT_COUNT = [sum(1 for x in OPTIONS if x[0] == b) for b in range(1, 8)]


def make_flows():
    flows = {}
    for step in range(3):
        for k in range(3):
            runs = []
            for o, (_, hops) in enumerate(OPTIONS):
                for h, (st, place, kk) in enumerate(hops):
                    if (st, kk) == (step, k):
                        runs.append((place, o, h))
            runs.sort(key=lambda run: (run[0], run[1]))
            flows[step, k] = runs
    return flows


FLOWS = make_flows()
X_ROW, LO_ROW, S_ROW, C_ROW, META_ROWS = 0, 16, 32, 48, 56
PLACE_LANES = 16


def plan_consts():
    hop = np.zeros((LANES, LANES), np.float32)
    group = np.zeros_like(hop)
    before = np.zeros_like(hop)
    dest = np.zeros((CHIPS, LANES), np.float32)
    first = np.zeros_like(dest)
    for o, (b, hops) in enumerate(OPTIONS):
        dest[b, o] = 1
        first[:, o] = o == OPT_BASE[b - 1]
        for step, place, k in hops:
            hop[o, place * PLACE_LANES + step * 3 + k] = 1
        for q, (bb, _) in enumerate(OPTIONS):
            if bb == b:
                group[o, q] = 1
                before[o, q] = o < q
    tri = np.triu(np.ones_like(hop), 1)
    return hop, hop.T.copy(), group, before, dest, first, tri


def plan_kernel(lens_ref, dest_ref, hop_ref, hop_t_ref, group_ref, before_ref, dmat_ref, first_ref, tri_ref, out_ref):
    plain = functools.partial(jnp.dot, preferred_element_type=F32)
    exact = functools.partial(plain, precision=lax.Precision.HIGHEST)
    shape = (CHIPS, LANES)
    row = lax.broadcasted_iota(I32, shape, 0)
    lane = lax.broadcasted_iota(I32, shape, 1)

    lens = lens_ref[...].reshape(CHIPS, 2 * LANES)
    lens = jnp.where(lane < SLOTS, lens[:, :LANES], pltpu.roll(lens[:, LANES:], SLOTS, 1))
    lens = jnp.where(lane < CHIP_SLOTS, lens, 0)
    flat = dest_ref[...]
    turned = pltpu.roll(flat, CHIP_SLOTS, 1)
    to = jnp.concatenate([(turned if c & 1 else flat)[c >> 1:(c >> 1) + 1] for c in range(CHIPS)], axis=0)
    rel = (to >> 6) ^ row
    half = (lens + 1) >> 1
    parts = [half.astype(F32), (lens - half).astype(F32)]

    def top_of(a):
        return jnp.max(jnp.max(a, axis=1, keepdims=True), axis=0, keepdims=True)

    tri = tri_ref[...].astype(BF)
    dmat = dmat_ref[...]
    demand = []
    for beta in range(2):
        mine = [jnp.where(rel == b, parts[beta], 0.0) for b in range(1, CHIPS)]
        earlier = plain(jnp.concatenate(mine, axis=0).astype(BF), tri)
        starts = jnp.zeros(shape, F32)
        total = jnp.zeros(shape, F32)
        for b in range(1, CHIPS):
            starts = jnp.where(rel == b, earlier[(b - 1) * CHIPS:b * CHIPS], starts)
            total = total + jnp.sum(mine[b - 1], axis=1, keepdims=True) * dmat[b:b + 1]
        demand.append(total)
        at = S_ROW + CHIPS * beta
        out_ref[at:at + CHIPS, :] = starts.astype(I32)

    def flip(a, bit):
        return jnp.where((row & bit) == 0, pltpu.roll(a, CHIPS - bit, 0), pltpu.roll(a, bit, 0))

    def link_loads(x, dot):
        y = dot(x, hop_ref[...])
        for bit in (4, 2, 1):
            y = y + flip(pltpu.roll(y, LANES - PLACE_LANES * bit, 1), bit)
            y = jnp.where(lane < PLACE_LANES * bit, y, 0.0)
        return y

    def path_cost(p):
        y = jnp.where(lane < PLACE_LANES, p, 0.0)
        for bit in (1, 2, 4):
            y = y + pltpu.roll(flip(y, bit), PLACE_LANES * bit, 1)
        return plain(y, hop_t_ref[...])

    both = demand[0] + demand[1]
    used = jnp.sum(dmat, axis=0, keepdims=True) > 0

    def norm(w):
        w = jnp.where(used, jnp.maximum(w, 1e-6), 0.0)
        return w / jnp.where(used, plain(w, group_ref[...]), 1.0)

    weight = norm(jnp.ones(shape, F32))
    best_top = jnp.full((1, 1), 3e38, F32)
    best = weight
    for _ in range(ITERS):
        loads = link_loads(weight * both, plain)
        top = top_of(loads)
        better = top < best_top
        best = jnp.where(better, weight, best)
        best_top = jnp.where(better, top, best_top)
        price = loads / jnp.maximum(top, 1.0)
        price = price * price
        weight = norm(weight * jnp.exp(-0.5 * path_cost(price * price)))

    top = jnp.zeros((1, 1), F32)
    for beta in range(2):
        total = demand[beta]
        x = jnp.minimum(jnp.floor(best * total * 0.995), total)
        x = x + first_ref[...] * (total - exact(x, group_ref[...]))
        top = jnp.maximum(top, top_of(link_loads(x, exact)))
        top = jnp.where(top_of(-x) > 0.0, 1e6, top)
        at = X_ROW + CHIPS * beta
        out_ref[at:at + CHIPS, :] = x.astype(I32)
        at = LO_ROW + CHIPS * beta
        out_ref[at:at + CHIPS, :] = exact(x, before_ref[...]).astype(I32)

    from_dev = 2 * row + (lane >> 5)
    to_dev = to >> 5
    crossing = jnp.where(from_dev == to_dev, 0.0, parts[0])
    come = jnp.zeros((1, 1), F32)
    for d in range(DEVS):
        here = jnp.sum(jnp.where(to_dev == d, crossing, 0.0), axis=1, keepdims=True)
        come = jnp.maximum(come, jnp.sum(here, axis=0, keepdims=True))
    pick = jnp.zeros((1, 1), I32)
    wide = jnp.zeros((1, 1), I32)
    for cap, rows in CLASSES:
        pick = pick + (top > cap).astype(I32)
        wide = wide + (come > rows).astype(I32)
    out_ref[C_ROW:C_ROW + CHIPS, :] = jnp.broadcast_to(jnp.maximum(pick, wide), shape)


def make_plan(lens_all, dest_slot):
    return pl.pallas_call(
        plan_kernel,
        out_shape=jax.ShapeDtypeStruct((META_ROWS, LANES), I32),
        name='plan',
    )(lens_all, dest_slot.reshape(KV, LANES), *plan_consts())


def gather_kernel(x_ref, out_ref, send_sem, recv_sem):
    me = lax.axis_index('dp')
    barrier = pltpu.get_barrier_semaphore()
    for r in range(1, DEVS):
        pl.semaphore_signal(barrier, inc=1, device_id=(lax.rem(me + r, DEVS),), device_id_type=pl.DeviceIdType.MESH)
    pl.semaphore_wait(barrier, DEVS - 1)
    copies = []
    for r in range(1, DEVS):
        copies.append(pltpu.make_async_remote_copy(
            src_ref=x_ref, dst_ref=out_ref.at[me], send_sem=send_sem.at[r], recv_sem=recv_sem.at[r],
            device_id=(lax.rem(me + r, DEVS),), device_id_type=pl.DeviceIdType.MESH))
        copies[-1].start()
    out_ref[me] = x_ref[...]
    for copy in copies:
        copy.wait()


def gather_lens(my_lens):
    row = jnp.pad(my_lens, (0, LANES - SLOTS)).reshape(1, LANES)
    return pl.pallas_call(
        gather_kernel,
        out_shape=jax.ShapeDtypeStruct((DEVS, 1, LANES), I32),
        in_specs=[VMEM], out_specs=VMEM,
        scratch_shapes=[pltpu.SemaphoreType.DMA((DEVS,))] * 2,
        compiler_params=pltpu.CompilerParams(collective_id=0, has_side_effects=True),
        name='gather_lens',
    )(row).reshape(DEVS, LANES)


def length(lens_ref, slot):
    return lens_ref[(slot >> 5) * LANES + (slot & 31)]


def part_of(m, beta):
    half = (m + 1) >> 1
    return (0, half) if beta == 0 else (half, m - half)


def row_copy(src, s0, dst, d0, n, sem):
    return pltpu.make_async_copy(src.at[pl.ds(s0, n)], dst.at[pl.ds(d0, n)], sem)


def drain(ref, n, sem):
    @pl.when(n > 0)
    def _():
        row_copy(ref, 0, ref, 0, n, sem).wait()


def pre_kernel(beta, dev_ref, lens_ref, dest_ref, k_ref, v_ref, out_ref, *rest):
    if beta == 0:
        src_ref, stage, sem = rest
    else:
        stage, sem = rest
    dev = dev_ref[0]
    core = dev & 1

    def one(i, q):
        slot = dev * SLOTS + i
        start, n = part_of(lens_ref[i], beta)
        moving = (dest_ref[slot] >> 5) != dev
        n = jnp.where(moving, n, 0)

        @pl.when(n > 0)
        def _():
            @pl.when(core == 0)
            def _():
                row_copy(v_ref, i * ROWS + start, stage, q, n, sem).start()

            @pl.when(core == 1)
            def _():
                row_copy(k_ref, i * ROWS + start, stage, q, n, sem).start()
        return q + n

    total = lax.fori_loop(0, SLOTS, one, I32(0))
    if beta == 0:
        def invert(i, _):
            for u in range(8):
                src_ref[dest_ref[i * 8 + u]] = i * 8 + u
            return 0
        lax.fori_loop(0, 64, invert, 0)
    drain(stage, total, sem)

    @pl.when(total > 0)
    def _():
        out = row_copy(stage, 0, out_ref, 0, total, sem)
        out.start()
        out.wait()


SMEM = pl.BlockSpec(memory_space=pltpu.SMEM)
ANY = pl.BlockSpec(memory_space=pltpu.HBM)
VMEM = pl.BlockSpec(memory_space=pltpu.VMEM)


def pre_pack(beta, dev, lens, dest, k, v):
    out = [jax.ShapeDtypeStruct((HALF, KV, DIM), BF)]
    specs = [ANY]
    if beta == 0:
        out.append(jax.ShapeDtypeStruct((TOTAL,), I32))
        specs.append(SMEM)
    return pl.pallas_call(
        functools.partial(pre_kernel, beta),
        out_shape=out, out_specs=specs,
        in_specs=[SMEM] * 3 + [ANY] * 2,
        scratch_shapes=[pltpu.VMEM((HALF, KV, DIM), BF), pltpu.SemaphoreType.DMA],
        compiler_params=pltpu.CompilerParams(vmem_limit_bytes=VMEM_LIMIT),
        cost_estimate=pl.CostEstimate(flops=100000000, bytes_accessed=12000000, transcendentals=0),
        name=f'pre_pack{beta}',
    )(dev, lens, dest, k, v)


class Table:
    def __init__(self, meta, chip, beta):
        self.meta, self.beta = meta, beta
        self.row = [(8 * beta + (chip ^ v)) * LANES for v in range(8)]

    def x(self, v, o):
        return self.meta[X_ROW * LANES + self.row[v] + o]

    def lo(self, v, o):
        return self.meta[LO_ROW * LANES + self.row[v] + o]

    def start(self, slot):
        return self.meta[S_ROW * 128 + (8 * self.beta + (slot >> 6)) * LANES + (slot & 63)]


def pack_kernel(beta, step, cap, dev_ref, meta, lens_ref, dest_ref, k_ref, v_ref, pre_ref, *rest):
    recv = {}
    n_in = 3 * step
    for q in range(n_in):
        recv[q // 3, q % 3] = rest[q]
    outs = rest[n_in:n_in + 3]
    stage, table_lo, table_hi, table_to, sem, sem_out = rest[n_in + 3:]
    dev = dev_ref[0]
    chip, core = dev >> 1, dev & 1
    plan = Table(meta, chip, beta)
    used = []
    count = I32(0)
    for k in range(3):
        where = I32(0)
        spans = {}
        for place, o, _ in FLOWS[step, k]:
            if place == 0:
                b = OPTIONS[o][0]
                n = plan.x(0, o)
                if b not in spans:
                    spans[b] = [plan.lo(0, o), I32(0), where]
                spans[b][1] = spans[b][1] + n
                where = where + n
        for b in range(1, 8):
            if b in spans:
                lo, n, to = spans[b]
                table_lo[b * 3 + k] = lo
                table_hi[b * 3 + k] = lo + n
                table_to[b * 3 + k] = to - lo + k * cap
            else:
                table_lo[b * 3 + k] = I32(0)
                table_hi[b * 3 + k] = I32(0)
                table_to[b * 3 + k] = I32(0)
        used.append(where)
        count = count + where

    if step > 0:
        came = {}
        for (st, kk), runs in FLOWS.items():
            if st < step:
                at = I32(0)
                for place, o, h in runs:
                    v = place ^ (1 << kk)
                    n = plan.x(v, o)
                    hops = OPTIONS[o][1]
                    if h + 1 < len(hops) and hops[h + 1][0] == step:
                        came[v, o] = (st, kk, at, n)
                    at = at + n
        for k in range(3):
            for place, o, h in FLOWS[step, k]:
                if place == 0:
                    continue
                st, kk, at, n = came[place, o]

                @pl.when(n > 0)
                def _(st=st, kk=kk, at=at, n=n, to=used[k], k=k):
                    row_copy(recv[st, kk], at, stage, to + k * cap, n, sem).start()
                used[k] = used[k] + n
                count = count + n

    def one(i, q):
        slot = chip * 64 + i
        to_slot = dest_ref[slot]
        mine = (i >> 5) == core
        start, n = part_of(length(lens_ref, slot), beta)
        b = chip ^ (to_slot >> 6)

        @pl.when(b > 0)
        def _():
            begin = plan.start(slot)
            for k in range(3):
                lo = jnp.maximum(begin, table_lo[b * 3 + k])
                hi = jnp.minimum(begin + n, table_hi[b * 3 + k])
                size = hi - lo
                to = table_to[b * 3 + k] + lo
                skip = lo - begin

                @pl.when(size > 0)
                def _():
                    home = (i & 31) * ROWS + start + skip

                    @pl.when(mine & (core == 0))
                    def _():
                        row_copy(k_ref, home, stage, to, size, sem).start()

                    @pl.when(mine & (core == 1))
                    def _():
                        row_copy(v_ref, home, stage, to, size, sem).start()

                    @pl.when(jnp.logical_not(mine))
                    def _():
                        row_copy(pre_ref, q + skip, stage, to, size, sem).start()
        away = jnp.logical_not(mine) & ((to_slot >> 5) != (slot >> 5))
        return q + jnp.where(away, n, 0)

    lax.fori_loop(0, 64, one, I32(0))
    drain(stage, count, sem)
    for k in range(3):
        @pl.when(used[k] > 0)
        def _(k=k):
            row_copy(stage, k * cap, outs[k], 0, used[k], sem_out.at[k]).start()
    for k in range(3):
        @pl.when(used[k] > 0)
        def _(k=k):
            row_copy(stage, k * cap, outs[k], 0, used[k], sem_out.at[k]).wait()


def pack(beta, step, cap, scalars, k, v, pre, recv):
    dev, meta, lens, dest, _ = scalars
    recv = [recv[q // 3, q % 3] for q in range(3 * step)]
    return pl.pallas_call(
        functools.partial(pack_kernel, beta, step, cap),
        out_shape=[jax.ShapeDtypeStruct((cap, KV, DIM), BF)] * 3,
        out_specs=[ANY] * 3,
        in_specs=[SMEM] * 4 + [ANY] * (3 + 3 * step),
        scratch_shapes=[pltpu.VMEM((3 * cap, KV, DIM), BF)] + [pltpu.SMEM((24,), I32)] * 3
        + [pltpu.SemaphoreType.DMA, pltpu.SemaphoreType.DMA((3,))],
        compiler_params=pltpu.CompilerParams(vmem_limit_bytes=VMEM_LIMIT),
        cost_estimate=pl.CostEstimate(flops=100000000, bytes_accessed=9000000, transcendentals=0),
        name=f'pack{step}{beta}',
    )(dev, meta, lens, dest, k, v, pre, *recv)


def arrivals(plan, table_lo, table_hi, table_at, base):
    for (st, kk), runs in FLOWS.items():
        at = I32(0)
        for place, o, h in runs:
            v = place ^ (1 << kk)
            n = plan.x(v, o)
            if h + 1 == len(OPTIONS[o][1]):
                lo = plan.lo(v, o)
                table_lo[base + o] = lo
                table_hi[base + o] = lo + n
                table_at[base + o] = at - lo
            at = at + n


def static_lookup(table, index):
    out = I32(table[0])
    for q in range(1, len(table)):
        out = jnp.where(index == q, I32(table[q]), out)
    return out


def fill_buffer_ids(buf_ref):
    for o, (_, hops) in enumerate(OPTIONS):
        buf_ref[o] = I32(hops[-1][0] * 3 + hops[-1][2])


def from_links(plan, chip, slot, n, tables, base, recv, dst, to, sem):
    table_lo, table_hi, table_at, buf_ref = tables
    b = chip ^ (slot >> 6)
    begin = plan.start(slot)
    first = static_lookup([0] + OPT_BASE, b)
    count = static_lookup([0] + OPT_COUNT, b)

    def piece(q, _):
        o = first + q
        lo = jnp.maximum(begin, table_lo[base + o])
        hi = jnp.minimum(begin + n, table_hi[base + o])
        size = hi - lo
        at = table_at[base + o] + lo
        put = to + lo - begin

        @pl.when(size > 0)
        def _():
            which = buf_ref[o]
            for w in range(9):
                @pl.when(which == w)
                def _(w=w):
                    row_copy(recv[w], at, dst, put, size, sem).start()
        return 0

    lax.fori_loop(0, count, piece, 0)


def post_kernel(beta, dev_ref, meta, lens_ref, src_ref, k_ref, v_ref, *rest):
    recv = rest[:9]
    out_ref, stage, table_lo, table_hi, table_at, buf_ref, sem = rest[9:]
    dev = dev_ref[0]
    chip, core = dev >> 1, dev & 1
    plan = Table(meta, chip, beta)
    arrivals(plan, table_lo, table_hi, table_at, 0)
    fill_buffer_ids(buf_ref)
    tables = (table_lo, table_hi, table_at, buf_ref)

    def one(j, q):
        slot = src_ref[(dev ^ 1) * SLOTS + j]
        start, n = part_of(length(lens_ref, slot), beta)
        owner = slot >> 5
        n = jnp.where(owner == (dev ^ 1), 0, n)

        @pl.when((owner == dev) & (n > 0))
        def _():
            home = (slot & 31) * ROWS + start

            @pl.when(core == 0)
            def _():
                row_copy(k_ref, home, stage, q, n, sem).start()

            @pl.when(core == 1)
            def _():
                row_copy(v_ref, home, stage, q, n, sem).start()

        @pl.when((owner >> 1) != chip)
        def _():
            from_links(plan, chip, slot, n, tables, 0, recv, stage, q, sem)
        return q + n

    total = lax.fori_loop(0, SLOTS, one, I32(0))
    drain(stage, total, sem)

    @pl.when(total > 0)
    def _():
        out = row_copy(stage, 0, out_ref, 0, total, sem)
        out.start()
        out.wait()


def post_pack(beta, rows, scalars, k, v, recv):
    dev, meta, lens, _, src = scalars
    recv = [recv[q // 3, q % 3] for q in range(9)]
    return pl.pallas_call(
        functools.partial(post_kernel, beta),
        out_shape=jax.ShapeDtypeStruct((rows, KV, DIM), BF),
        out_specs=ANY,
        in_specs=[SMEM] * 4 + [ANY] * 11,
        scratch_shapes=[pltpu.VMEM((rows, KV, DIM), BF)] + [pltpu.SMEM((40,), I32)] * 4
        + [pltpu.SemaphoreType.DMA],
        compiler_params=pltpu.CompilerParams(vmem_limit_bytes=VMEM_LIMIT),
        cost_estimate=pl.CostEstimate(flops=100000000, bytes_accessed=12000000, transcendentals=0),
        name=f'post_pack{beta}',
    )(dev, meta, lens, src, k, v, *recv)


N_BUF, AHEAD = 6, 4
GROUP_ROWS = 64


def final_kernel(dev_ref, meta, lens_ref, dest_ref, src_ref, k_ref, v_ref, *rest):
    pre, post = rest[0:2], rest[2:4]
    recv = [rest[4:13], rest[13:22]]
    q_ref, kn_ref, vn_ref, attn_ref, ko_ref, vo_ref, lens_out = rest[22:29]
    kbuf, vbuf, zeros, cols, table_lo, table_hi, table_at, buf_ref, pre_at, post_at, sem_in, sem_out = rest[29:]
    dev = dev_ref[0]
    chip, core = dev >> 1, dev & 1
    plans = [Table(meta, chip, beta) for beta in range(2)]
    for beta in range(2):
        arrivals(plans[beta], table_lo, table_hi, table_at, 40 * beta)
    fill_buffer_ids(buf_ref)
    tables = (table_lo, table_hi, table_at, buf_ref)

    def offsets(i, carry):
        a0, a1, b0, b1 = carry
        slot = (dev ^ 1) * SLOTS + i
        m = length(lens_ref, slot)
        pre_at[i], pre_at[SLOTS + i] = a0, a1
        away = (dest_ref[slot] >> 5) != (dev ^ 1)
        half = (m + 1) >> 1
        a0 = a0 + jnp.where(away, half, 0)
        a1 = a1 + jnp.where(away, m - half, 0)
        slot = src_ref[dev * SLOTS + i]
        m = length(lens_ref, slot)
        post_at[i], post_at[SLOTS + i] = b0, b1
        lens_out[i] = m + 1
        moved = (slot >> 5) != dev
        half = (m + 1) >> 1
        b0 = b0 + jnp.where(moved, half, 0)
        b1 = b1 + jnp.where(moved, m - half, 0)
        return a0, a1, b0, b1

    zero = I32(0)
    lax.fori_loop(0, SLOTS, offsets, (zero, zero, zero, zero))

    def fetch(j):
        slot = src_ref[dev * SLOTS + j]
        m = length(lens_ref, slot)
        owner = slot >> 5
        buf = j % N_BUF
        kb, vb = kbuf.at[buf], vbuf.at[buf]
        sk, sv = sem_in.at[0, buf], sem_in.at[1, buf]

        @pl.when(owner == dev)
        def _():
            home = (slot & 31) * ROWS
            row_copy(k_ref, home, kb, 0, m, sk).start()
            row_copy(v_ref, home, vb, 0, m, sv).start()

        @pl.when(owner != dev)
        def _():
            for beta in range(2):
                start, n = part_of(m, beta)

                def lane(dst, sem, other, other_sem):
                    @pl.when((owner >> 1) == chip)
                    def _():
                        row_copy(pre[beta], pre_at[SLOTS * beta + (slot & 31)], dst, start, n, sem).start()

                    @pl.when((owner >> 1) != chip)
                    def _():
                        from_links(plans[beta], chip, slot, n, tables, 40 * beta, recv[beta], dst, start, sem)
                    row_copy(post[beta], post_at[SLOTS * beta + j], other, start, n, other_sem).start()

                @pl.when(core == 0)
                def _():
                    lane(kb, sk, vb, sv)

                @pl.when(core == 1)
                def _():
                    lane(vb, sv, kb, sk)

    def emit(j, m):
        buf = j % N_BUF
        for ref, out, q in ((kbuf, ko_ref, 0), (vbuf, vo_ref, 1)):
            row_copy(ref.at[buf], 0, out, j * ROWS, m + 1, sem_out.at[q, buf]).start()

            @pl.when(m + 1 < ROWS)
            def _():
                row_copy(zeros, 0, out, j * ROWS + m + 1, ROWS - 1 - m, sem_out.at[q, buf]).start()

    def emitted(j):
        buf = j % N_BUF
        row_copy(kbuf.at[buf], 0, ko_ref, j * ROWS, ROWS, sem_out.at[0, buf]).wait()
        row_copy(vbuf.at[buf], 0, vo_ref, j * ROWS, ROWS, sem_out.at[1, buf]).wait()

    def clear(t, _):
        for n in range(N_BUF):
            vbuf[n, pl.ds(t * GROUP_ROWS, GROUP_ROWS)] = jnp.zeros((GROUP_ROWS, KV, DIM), BF)
        zeros[pl.ds(t * GROUP_ROWS, GROUP_ROWS)] = jnp.zeros((GROUP_ROWS, KV, DIM), BF)
        return 0
    lax.fori_loop(0, ROWS // GROUP_ROWS, clear, 0)

    def begin(j, _):
        fetch(j)
        return 0
    lax.fori_loop(0, AHEAD, begin, 0)
    head = lax.broadcasted_iota(I32, cols.shape, 0) // GROUP
    col = lax.broadcasted_iota(I32, cols.shape, 1)
    cols[...] = jnp.where(head == (col & (KV - 1)), col, LAST)

    def pair(jj, _):
        def prefetch(u, _):
            ahead = 2 * jj + u + AHEAD

            @pl.when(ahead < SLOTS)
            def _():
                @pl.when(ahead >= N_BUF)
                def _():
                    emitted(ahead - N_BUF)
                fetch(ahead)
            return 0
        lax.fori_loop(0, 2, prefetch, 0)
        work = []
        for u in range(2):
            j = 2 * jj + u
            m = length(lens_ref, src_ref[dev * SLOTS + j])
            buf = j % N_BUF
            row_copy(k_ref, 0, kbuf.at[buf], 0, m, sem_in.at[0, buf]).wait()
            row_copy(v_ref, 0, vbuf.at[buf], 0, m, sem_in.at[1, buf]).wait()
            kbuf[buf, m] = kn_ref[j]
            vbuf[buf, m] = vn_ref[j]
            emit(j, m)
            work.append((j, m, buf))
        scores = []
        for j, m, buf in work:
            kk = kbuf[buf].reshape(KV * ROWS, DIM)
            s = lax.dot_general(q_ref[j], kk, (((1,), (1,)), ((), ())), preferred_element_type=F32)
            scores.append(jnp.where(cols[...] < KV * (m + 1), s * (DIM ** -0.5), -1e30))
        for (j, m, buf), s in zip(work, scores):
            p = jnp.exp(s - jnp.max(s, axis=1, keepdims=True))
            l = jnp.sum(p, axis=1, keepdims=True)
            vv = vbuf[buf].reshape(KV * ROWS, DIM)
            acc = jnp.dot(p.astype(BF), vv, preferred_element_type=F32)
            attn_ref[j] = (acc / l).astype(BF)
        return 0

    lax.fori_loop(0, SLOTS // 2, pair, 0)

    def last(j, _):
        emitted(j)
        return 0
    lax.fori_loop(SLOTS - N_BUF, SLOTS, last, 0)


def finish(scalars, k, v, pre, post, recv, query, k_new, v_new):
    flat = [recv[beta][q // 3, q % 3] for beta in range(2) for q in range(9)]
    return pl.pallas_call(
        final_kernel,
        out_shape=[jax.ShapeDtypeStruct((SLOTS, HEADS, DIM), BF)]
        + [jax.ShapeDtypeStruct((SLOTS * ROWS, KV, DIM), BF)] * 2 + [jax.ShapeDtypeStruct((SLOTS,), I32)],
        out_specs=[VMEM, ANY, ANY, SMEM],
        in_specs=[SMEM] * len(scalars) + [ANY] * (6 + len(flat)) + [VMEM] * 3,
        scratch_shapes=[pltpu.VMEM((N_BUF, ROWS, KV, DIM), BF)] * 2
        + [pltpu.VMEM((ROWS, KV, DIM), BF), pltpu.VMEM((HEADS, KV * ROWS), I32)]
        + [pltpu.SMEM((80,), I32)] * 3 + [pltpu.SMEM((40,), I32)] + [pltpu.SMEM((64,), I32)] * 2
        + [pltpu.SemaphoreType.DMA((2, N_BUF))] * 2,
        compiler_params=pltpu.CompilerParams(vmem_limit_bytes=VMEM_LIMIT),
        cost_estimate=pl.CostEstimate(flops=1000000000, bytes_accessed=67000000, transcendentals=0),
        name='finish',
    )(*scalars, k, v, *pre, *post, *flat, query, k_new, v_new)


def swap(x, mask):
    return lax.ppermute(x, 'dp', [(i, i ^ mask) for i in range(DEVS)])


def routed(caps, scalars, k, v, pre0, pre1_send, query, k_new, v_new):
    cap, rows = caps
    recv = [{}, {}]
    pre = [pre0, None]
    for step in range(3):
        for beta in range(2):
            if step == 0 and beta == 1:
                pre[1] = swap(pre1_send, 1)
            sends = pack(beta, step, cap, scalars, k, v, pre[beta], recv[beta])
            for dim in range(3):
                recv[beta][step, dim] = swap(sends[dim], 2 << dim)
    post = [swap(post_pack(beta, rows, scalars, k, v, recv[beta]), 1) for beta in range(2)]
    return finish(scalars, k, v, pre, post, recv, query, k_new, v_new)


def ring_move(k, v, source_of):
    me = lax.axis_index('dp')
    shift = [(i, (i + 1) % 16) for i in range(16)]

    pick = source_of & 31

    def take(r, kh, vh, ka, va):
        here = ((source_of >> 5) == (me - r) % 16)[:, None, None, None]
        return jnp.where(here, kh[pick], ka), jnp.where(here, vh[pick], va)

    def turn(r, carry):
        kh, vh, ka, va = carry
        ka, va = take(r, kh, vh, ka, va)
        return lax.ppermute(kh, 'dp', shift), lax.ppermute(vh, 'dp', shift), ka, va

    ka, va = take(0, k, v, jnp.zeros_like(k), jnp.zeros_like(v))
    first = (lax.ppermute(k, 'dp', shift), lax.ppermute(v, 'dp', shift), ka, va)
    _, _, ka, va = lax.fori_loop(1, 16, turn, first)
    return ka, va


def write_new(moved, new_rows, lens_new):
    positions = jnp.arange(ROWS, dtype=I32)
    keep_row = (positions[None, :] < lens_new[:, None])[:, :, None, None]
    at_new = (positions[None, :] == lens_new[:, None])[:, :, None, None]
    return jnp.where(keep_row, moved, jnp.where(at_new, new_rows[:, None], jnp.zeros((), moved.dtype)))


def attend(query, k_full, v_full, lens_new):
    q_grp = query.reshape(SLOTS, KV, GROUP, DIM)
    scores = jnp.einsum('rkgd,rtkd->rkgt', q_grp, k_full, preferred_element_type=F32) * (DIM ** -0.5)
    positions = jnp.arange(ROWS, dtype=I32)
    valid_pos = (positions[None, :] <= lens_new[:, None])[:, None, None, :]
    scores = jnp.where(valid_pos, scores, -1e30)
    weights = jnp.exp(scores - jnp.max(scores, axis=-1, keepdims=True))
    prob_sum = jnp.sum(weights, axis=-1, keepdims=True)
    acc = jnp.einsum('rkgt,rtkd->rkgd', weights.astype(BF), v_full, preferred_element_type=F32) / prob_sum
    return acc.astype(BF).reshape(SLOTS, HEADS, DIM)


def solution(mesh):
    def local(query, k_cache, v_cache, cache_lens, dest_slot, k_new, v_new):
        me = lax.axis_index('dp')
        dev = me.reshape(1).astype(I32)
        flat, full = (SLOTS * ROWS, KV, DIM), (SLOTS, ROWS, KV, DIM)
        k, v = k_cache.reshape(flat), v_cache.reshape(flat)
        lens = gather_lens(cache_lens)
        pre_send, src = pre_pack(0, dev, cache_lens, dest_slot, k, v)
        pre0 = swap(pre_send, 1)
        pre1_send, = pre_pack(1, dev, cache_lens, dest_slot, k, v)
        plan = make_plan(lens, dest_slot)
        scalars = (dev, plan.reshape(-1), lens.reshape(-1), dest_slot, src)

        def fast(caps, args):
            return tuple(routed(caps, *args))

        def slow(args):
            (_, _, lens, _, src), k, v, _, _, query, k_new, v_new = args
            source_of = lax.dynamic_slice(src, (me * SLOTS,), (SLOTS,))
            lens_new = length(lens, source_of)
            ka, va = ring_move(k.reshape(full), v.reshape(full), source_of)
            ka = write_new(ka, k_new, lens_new)
            va = write_new(va, v_new, lens_new)
            attn = attend(query, ka, va, lens_new)
            return attn, ka.reshape(flat), va.reshape(flat), lens_new + 1

        branches = [functools.partial(fast, caps) for caps in CLASSES] + [slow]
        attn, ko, vo, lens_out = lax.switch(
            plan[C_ROW, 0], branches, (scalars, k, v, pre0, pre1_send, query, k_new, v_new))
        return attn, ko.reshape(full), vo.reshape(full), lens_out

    row_spec = P('dp')
    return jax.shard_map(local, mesh=mesh, in_specs=(row_spec, row_spec, row_spec, row_spec, P(), row_spec, row_spec), out_specs=(row_spec, row_spec, row_spec, row_spec), check_vma=False)
```

```python
import functools
import itertools

import jax
import jax.numpy as jnp
import numpy as np
from jax import lax
from jax.experimental import pallas as pl
from jax.experimental.pallas import tpu as pltpu
from jax.sharding import PartitionSpec as P


I32, F32, BF = jnp.int32, jnp.float32, jnp.bfloat16
DEVS, SLOTS, TOTAL = 16, 32, 512
CHIPS, CHIP_SLOTS = 8, 64
DESTS = range(1, CHIPS)
ROWS = 512
HEADS, KV, DIM, GROUP = 28, 4, 128, 7
LANES = 128
BATCHES = (0, 1)
PRE = 6912
POST = 6656
HALF = ROWS // 2
CLASSES = (2224, 2552, 2752, 2984, 3176, 3400, 3592, 4600)
ITERS = 12
FIRST_STEP, SHRINK = 1.5, 15 ** (-1 / 11)
LAST = jnp.iinfo(jnp.int32).max
VMEM_LIMIT = 62914560
TABLES = 40


def make_options():
    found = []
    for b in DESTS:
        dims = [k for k in range(3) if (b >> k) & 1]
        mine = []
        for steps in itertools.combinations(range(3), len(dims)):
            for order in itertools.permutations(dims):
                place, hops = 0, []
                for step, k in zip(steps, order):
                    hops.append((step, place, k))
                    place ^= 1 << k
                mine.append((b, tuple(hops)))
        mine.sort(key=lambda option: (option[1][0][0], option[1][0][2], option[1]))
        found += mine
    return found


OPTIONS = make_options()
N_OPT = len(OPTIONS)
OPT_BASE = [next(o for o in range(N_OPT) if OPTIONS[o][0] == b) for b in DESTS]
OPT_COUNT = [sum(1 for x in OPTIONS if x[0] == b) for b in DESTS]


def make_flows():
    flows = {}
    for step in range(3):
        for k in range(3):
            runs = []
            for o, (_, hops) in enumerate(OPTIONS):
                for h, (st, place, kk) in enumerate(hops):
                    if (st, kk) == (step, k):
                        runs.append((place, o, h))
            runs.sort(key=lambda run: (run[0], run[1]))
            flows[step, k] = runs
    return flows


FLOWS = make_flows()
X_ROW, LO_ROW, S_ROW, C_ROW, META_ROWS = 0, 16, 32, 48, 56
PLACE_LANES = 16
BITS = (1, 2, 4)


def caps_of(rows):
    return rows // 2


def plan_consts():
    hop = np.zeros((LANES, LANES), np.float32)
    group = np.zeros_like(hop)
    before = np.zeros_like(hop)
    dest = np.zeros((CHIPS, LANES), np.float32)
    first = np.zeros_like(dest)
    for o, (b, hops) in enumerate(OPTIONS):
        dest[b, o] = 1
        first[:, o] = o == OPT_BASE[b - 1]
        for step, place, k in hops:
            hop[o, place * PLACE_LANES + step * 3 + k] = 1
        for q, (bb, _) in enumerate(OPTIONS):
            if bb == b:
                group[o, q] = 1
                before[o, q] = o < q
    tri = np.triu(np.ones_like(hop), 1)
    return hop, hop.T.copy(), group, before, dest, first, tri


def plan_kernel(lens_ref, dest_ref, hop_ref, hop_t_ref, group_ref, before_ref, dmat_ref, first_ref, tri_ref, out_ref):
    exact = functools.partial(jnp.dot, preferred_element_type=F32, precision=lax.Precision.HIGHEST)

    def plain(a, b):
        return jnp.dot(a.astype(BF), b.astype(BF), preferred_element_type=F32)

    shape = (CHIPS, LANES)
    row = lax.broadcasted_iota(I32, shape, 0)
    lane = lax.broadcasted_iota(I32, shape, 1)

    lens = lens_ref[...].reshape(CHIPS, 2 * LANES)
    lens = jnp.where(lane < SLOTS, lens[:, :LANES], pltpu.roll(lens[:, LANES:], SLOTS, 1))
    lens = jnp.where(lane < CHIP_SLOTS, lens, 0)
    flat = dest_ref[...]
    turned = pltpu.roll(flat, CHIP_SLOTS, 1)
    to = jnp.concatenate([(turned if c & 1 else flat)[c >> 1:(c >> 1) + 1] for c in range(CHIPS)], axis=0)
    rel = (to >> 6) ^ row
    early = (lens + 1) >> 1
    parts = [early.astype(F32), (lens - early).astype(F32)]

    def top_of(a):
        return jnp.max(jnp.max(a, axis=1, keepdims=True), axis=0, keepdims=True)

    tri = tri_ref[...]
    dmat = dmat_ref[...]
    demand = []
    for beta in range(2):
        mine = [jnp.where(rel == b, parts[beta], 0.0) for b in DESTS]
        earlier = plain(jnp.concatenate(mine, axis=0), tri)
        starts = jnp.zeros(shape, F32)
        total = jnp.zeros(shape, F32)
        for b in DESTS:
            starts = jnp.where(rel == b, earlier[(b - 1) * CHIPS:b * CHIPS], starts)
            total = total + jnp.sum(mine[b - 1], axis=1, keepdims=True) * dmat[b:b + 1]
        demand.append(total)
        at = S_ROW + CHIPS * beta
        out_ref[at:at + CHIPS, :] = starts.astype(I32)

    def flip(a, bit):
        return jnp.where((row & bit) == 0, pltpu.roll(a, CHIPS - bit, 0), pltpu.roll(a, bit, 0))

    def link_loads(x, dot):
        y = dot(x, hop_ref[...])
        for bit in BITS[::-1]:
            y = y + flip(pltpu.roll(y, LANES - PLACE_LANES * bit, 1), bit)
            y = jnp.where(lane < PLACE_LANES * bit, y, 0.0)
        return y

    def path_cost(p):
        y = jnp.where(lane < PLACE_LANES, p, 0.0)
        for bit in BITS:
            y = y + pltpu.roll(flip(y, bit), PLACE_LANES * bit, 1)
        return plain(y, hop_t_ref[...])

    both = demand[0] + demand[1]
    used = jnp.sum(dmat, axis=0, keepdims=True) > 0

    def norm(w):
        w = jnp.where(used, jnp.maximum(w, 1e-6), 0.0)
        return w / jnp.where(used, plain(w, group_ref[...]), 1.0)

    weight = norm(jnp.ones(shape, F32))

    def improve(_, carry):
        weight, best, best_top, size = carry
        loads = link_loads(weight * both, plain)
        top = top_of(loads)
        better = top < best_top
        best = jnp.where(better, weight, best)
        best_top = jnp.where(better, top, best_top)
        price = loads / jnp.maximum(top, 1.0)
        for _ in BITS:
            price = price * price
        return norm(weight * jnp.exp(-size * path_cost(price))), best, best_top, size * SHRINK

    start = (weight, weight, jnp.full((1, 1), 3e38, F32), jnp.full((1, 1), FIRST_STEP, F32))
    best = lax.fori_loop(0, ITERS, improve, start)[1]

    pick = jnp.zeros((1, 1), I32)
    for t in range(2):
        total = demand[t]
        x = jnp.minimum(jnp.floor(best * total * 0.995), total)
        x = x + first_ref[...] * (total - exact(x, group_ref[...]))
        top = top_of(link_loads(x, exact))
        top = jnp.where(top_of(-x) > 0.0, 1e6, top)
        need = jnp.zeros((1, 1), I32)
        for rows in CLASSES:
            need = need + (top > caps_of(rows)).astype(I32)
        pick = jnp.maximum(pick, need)
        at = X_ROW + CHIPS * t
        out_ref[at:at + CHIPS, :] = x.astype(I32)
        at = LO_ROW + CHIPS * t
        out_ref[at:at + CHIPS, :] = exact(x, before_ref[...]).astype(I32)

    from_dev = 2 * row + (lane >> 5)
    to_dev = to >> 5
    crossing = jnp.where(from_dev == to_dev, 0.0, parts[0])
    come = jnp.concatenate([jnp.where(to_dev == d, crossing, 0.0) for d in range(DEVS)], axis=0)
    come = plain(come, jnp.ones((LANES, LANES), F32)).reshape(DEVS, CHIPS, LANES)
    over = top_of(jnp.sum(come, axis=1)) - POST
    for core in range(2):
        leave = jnp.where((lane >> 5) == core, crossing, 0.0)
        over = jnp.maximum(over, top_of(jnp.sum(leave, axis=1, keepdims=True)) - PRE)
    pick = jnp.where(over > 0.0, len(CLASSES), pick)
    out_ref[C_ROW:C_ROW + CHIPS, :] = jnp.broadcast_to(pick, shape)


def make_plan(lens_all, dest_slot):
    return pl.pallas_call(
        plan_kernel,
        out_shape=jax.ShapeDtypeStruct((META_ROWS, LANES), I32),
        name='plan',
    )(lens_all, dest_slot.reshape(KV, LANES), *plan_consts())


def gather_kernel(x_ref, out_ref, send_sem, recv_sem):
    me = lax.axis_index('dp')
    barrier = pltpu.get_barrier_semaphore()
    for r in range(1, DEVS):
        pl.semaphore_signal(barrier, inc=1, device_id=(lax.rem(me + r, DEVS),), device_id_type=pl.DeviceIdType.MESH)
    pl.semaphore_wait(barrier, DEVS - 1)
    copies = []
    for r in range(1, DEVS):
        copies.append(pltpu.make_async_remote_copy(
            src_ref=x_ref, dst_ref=out_ref.at[me], send_sem=send_sem.at[r], recv_sem=recv_sem.at[r],
            device_id=(lax.rem(me + r, DEVS),), device_id_type=pl.DeviceIdType.MESH))
        copies[-1].start()
    out_ref[me] = x_ref[...]
    for copy in copies:
        copy.wait()


def gather_lens(my_lens):
    row = jnp.pad(my_lens, (0, LANES - SLOTS)).reshape(1, LANES)
    return pl.pallas_call(
        gather_kernel,
        out_shape=jax.ShapeDtypeStruct((DEVS, 1, LANES), I32),
        in_specs=[VMEM], out_specs=VMEM,
        scratch_shapes=[pltpu.SemaphoreType.DMA((DEVS,))] * 2,
        compiler_params=pltpu.CompilerParams(collective_id=0, has_side_effects=True),
        name='gather_lens',
    )(row).reshape(DEVS, LANES)


def length(lens_ref, slot):
    return lens_ref[(slot >> 5) * LANES + (slot & 31)]


def part_of(m, beta):
    early = (m + 1) >> 1
    return (0, early)[beta], (early, m - early)[beta]


def row_copy(src, s0, dst, d0, n, sem):
    return pltpu.make_async_copy(src.at[pl.ds(s0, n)], dst.at[pl.ds(d0, n)], sem)


def drain(ref, n, sem):
    @pl.when(n > 0)
    def _():
        row_copy(ref, 0, ref, 0, n, sem).wait()


def flush(stage, s0, out, n, sem):
    @pl.when(n > 0)
    def _():
        copy = row_copy(stage, s0, out, 0, n, sem)
        copy.start()
        copy.wait()


def start_copy(core, flip, k_ref, v_ref, s0, dst, d0, n, sem):
    for c, ref in enumerate((v_ref, k_ref) if flip else (k_ref, v_ref)):
        @pl.when(core == c)
        def _(ref=ref):
            row_copy(ref, s0, dst, d0, n, sem).start()


SMEM = pl.BlockSpec(memory_space=pltpu.SMEM)
ANY = pl.BlockSpec(memory_space=pltpu.HBM)
VMEM = pl.BlockSpec(memory_space=pltpu.VMEM)


def rows_of(n, dtype=BF):
    return jax.ShapeDtypeStruct((n, KV, DIM), dtype)


def local_call(kernel, **kwargs):
    return pl.pallas_call(
        kernel, compiler_params=pltpu.CompilerParams(vmem_limit_bytes=VMEM_LIMIT), **kwargs)


def pre_kernel(beta, with_src, dev_ref, lens_ref, dest_ref, k_ref, v_ref, out_ref, *rest):
    if with_src:
        src_ref, stage, sem = rest
    else:
        stage, sem = rest
    dev = dev_ref[0]
    core = dev & 1

    def one(i, q):
        start, n = part_of(lens_ref[i], beta)
        moving = (dest_ref[dev * SLOTS + i] >> 5) != dev
        n = jnp.where(moving, n, 0)

        @pl.when(n > 0)
        def _():
            start_copy(core, True, k_ref, v_ref, i * ROWS + start, stage, q, n, sem)

        return q + n

    total = lax.fori_loop(0, SLOTS, one, I32(0))
    if with_src:
        def invert(i, _):
            for u in range(CHIPS):
                at = i * CHIPS + u
                src_ref[dest_ref[at]] = at
            return 0

        lax.fori_loop(0, TOTAL // CHIPS, invert, 0)
    drain(stage, total, sem)
    flush(stage, 0, out_ref, jnp.minimum(total, PRE), sem)


def pre_pack(beta, with_src, dev, lens, dest, k, v):
    out, specs = [rows_of(PRE)], [ANY]
    if with_src:
        out.append(jax.ShapeDtypeStruct((TOTAL,), I32))
        specs.append(SMEM)
    got = local_call(
        functools.partial(pre_kernel, beta, with_src),
        out_shape=out, out_specs=specs, in_specs=[SMEM] * 3 + [ANY] * 2,
        scratch_shapes=[pltpu.VMEM((SLOTS * HALF, KV, DIM), BF), pltpu.SemaphoreType.DMA],
    )(dev, lens, dest, k, v)
    return got if with_src else got[0]


class Table:
    def __init__(self, meta, chip, beta):
        self.meta, self.at = meta, CHIPS * BATCHES[beta]
        self.row = [(self.at + (chip ^ v)) * LANES for v in range(CHIPS)]

    def x(self, v, o):
        return self.meta[X_ROW * LANES + self.row[v] + o]

    def lo(self, v, o):
        return self.meta[LO_ROW * LANES + self.row[v] + o]

    def start(self, slot):
        return self.meta[S_ROW * LANES + (self.at + (slot // CHIP_SLOTS)) * LANES + (slot & 63)]


def pack_kernel(beta, step, cap, dev_ref, meta, lens_ref, dest_ref, k_ref, v_ref, pre_ref, *rest):
    recv = {}
    n_in = 3 * step
    for q in range(n_in):
        recv[q // 3, q % 3] = rest[q]
    outs = rest[n_in:n_in + 3]
    stage, table_lo, table_hi, table_to, sem, sem_out = rest[n_in + 3:]
    dev = dev_ref[0]
    chip, core = dev >> 1, dev & 1
    plan = Table(meta, chip, beta)
    used = []
    count = I32(0)
    for k in range(3):
        where = I32(0)
        spans = {}
        for place, o, _ in FLOWS[step, k]:
            if place == 0:
                b = OPTIONS[o][0]
                n = plan.x(0, o)
                if b not in spans:
                    spans[b] = [plan.lo(0, o), I32(0), where]
                spans[b][1] = spans[b][1] + n
                where = where + n
        for b in DESTS:
            if b in spans:
                lo, n, to = spans[b]
                table_lo[b * 3 + k] = lo
                table_hi[b * 3 + k] = lo + n
                table_to[b * 3 + k] = to - lo + k * cap
            else:
                table_lo[b * 3 + k] = I32(0)
                table_hi[b * 3 + k] = I32(0)
                table_to[b * 3 + k] = I32(0)
        used.append(where)
        count = count + where

    if step > 0:
        came = {}
        for (st, kk), runs in FLOWS.items():
            if st < step:
                at = I32(0)
                for place, o, h in runs:
                    v = place ^ (1 << kk)
                    n = plan.x(v, o)
                    hops = OPTIONS[o][1]
                    if h + 1 < len(hops) and hops[h + 1][0] == step:
                        came[v, o] = (st, kk, at, n)
                    at = at + n
        for k in range(3):
            for place, o, h in FLOWS[step, k]:
                if place == 0:
                    continue
                st, kk, at, n = came[place, o]

                @pl.when(n > 0)
                def _(st=st, kk=kk, at=at, n=n, to=used[k], k=k):
                    row_copy(recv[st, kk], at, stage, to + k * cap, n, sem).start()

                used[k] = used[k] + n
                count = count + n

    def one(i, q):
        slot = chip * 64 + i
        to_slot = dest_ref[slot]
        mine = (i >> 5) == core
        start, n = part_of(length(lens_ref, slot), beta)
        b = chip ^ (to_slot >> 6)

        @pl.when(b > 0)
        def _():
            begin = plan.start(slot)
            for k in range(3):
                lo = jnp.maximum(begin, table_lo[b * 3 + k])
                hi = jnp.minimum(begin + n, table_hi[b * 3 + k])
                size = hi - lo
                to = table_to[b * 3 + k] + lo
                skip = lo - begin

                @pl.when(size > 0)
                def _():
                    home = (i & 31) * ROWS + start + skip

                    @pl.when(mine)
                    def _():
                        start_copy(core, False, k_ref, v_ref, home, stage, to, size, sem)

                    @pl.when(jnp.logical_not(mine))
                    def _():
                        row_copy(pre_ref, q + skip, stage, to, size, sem).start()

        away = jnp.logical_not(mine) & ((to_slot >> 5) != (slot >> 5))
        return q + jnp.where(away, n, 0)

    lax.fori_loop(0, 64, one, I32(0))
    drain(stage, count, sem)
    for k in range(3):
        @pl.when(used[k] > 0)
        def _(k=k):
            row_copy(stage, k * cap, outs[k], 0, used[k], sem_out.at[k]).start()
    for k in range(3):
        @pl.when(used[k] > 0)
        def _(k=k):
            row_copy(stage, k * cap, outs[k], 0, used[k], sem_out.at[k]).wait()


def pack(beta, step, cap, scalars, k, v, pre, recv):
    dev, meta, lens, dest, _ = scalars
    recv = [recv[q // 3, q % 3] for q in range(3 * step)]
    return local_call(
        functools.partial(pack_kernel, beta, step, cap),
        out_shape=[rows_of(cap)] * 3, out_specs=[ANY] * 3,
        in_specs=[SMEM] * 4 + [ANY] * (3 + len(recv)),
        scratch_shapes=[pltpu.VMEM((3 * cap, KV, DIM), BF)] + [pltpu.SMEM((TABLES,), I32)] * 3
        + [pltpu.SemaphoreType.DMA, pltpu.SemaphoreType.DMA((3,))],
    )(dev, meta, lens, dest, k, v, pre, *recv)


def table_kernel(dev_ref, meta, lo_ref, hi_ref, at_ref, buf_ref):
    for beta in BATCHES:
        plan = Table(meta, dev_ref[0] >> 1, beta)
        base = TABLES * beta
        for (st, kk), runs in FLOWS.items():
            at = I32(0)
            for place, o, h in runs:
                v = place ^ (1 << kk)
                n = plan.x(v, o)
                if h + 1 == len(OPTIONS[o][1]):
                    lo = plan.lo(v, o)
                    lo_ref[base + o] = lo
                    hi_ref[base + o] = lo + n
                    at_ref[base + o] = at - lo
                    buf_ref[base + o] = I32(st * 3 + kk)
                at = at + n


def arrivals(dev, meta):
    return local_call(
        table_kernel, out_shape=[jax.ShapeDtypeStruct((2 * TABLES,), I32)] * 4,
        out_specs=[SMEM] * 4, in_specs=[SMEM] * 2)(dev, meta)


def static_lookup(table, index):
    out = I32(table[0])
    for q in range(1, len(table)):
        out = jnp.where(index == q, I32(table[q]), out)
    return out


def from_links(plan, chip, slot, n, tables, base, recv, dst, to, sem):
    table_lo, table_hi, table_at, buf_ref = tables
    b = chip ^ (slot // CHIP_SLOTS)
    begin = plan.start(slot)
    first = static_lookup([0] + OPT_BASE, b)
    count = static_lookup([0] + OPT_COUNT, b)

    def piece(q, _):
        o = first + q
        lo = jnp.maximum(begin, table_lo[base + o])
        hi = jnp.minimum(begin + n, table_hi[base + o])
        size = hi - lo
        at = table_at[base + o] + lo
        put = to + lo - begin

        @pl.when(size > 0)
        def _():
            which = buf_ref[base + o]
            for w in range(9):
                @pl.when(which == w)
                def _(w=w):
                    row_copy(recv[w], at, dst, put, size, sem).start()

        return 0

    lax.fori_loop(0, count, piece, 0)


def post_kernel(beta, other, dev_ref, meta, lens_ref, dest_ref, src_ref, *rest):
    tables, (k_ref, v_ref, pre_ref, *recv), (out_ref, stage, pre_at, sem) = rest[:4], rest[4:16], rest[16:]
    dev = dev_ref[0]
    chip, core = dev >> 1, dev & 1
    plan = Table(meta, chip, beta)
    sibling = dev ^ 1
    target = sibling if other else dev

    if not other:
        def place(i, q):
            pre_at[i] = q
            slot = sibling * SLOTS + i
            _, n = part_of(length(lens_ref, slot), beta)
            return q + jnp.where((dest_ref[slot] >> 5) != sibling, n, 0)

        lax.fori_loop(0, SLOTS, place, I32(0))

    def one(j, q):
        slot = src_ref[target * SLOTS + j]
        start, n = part_of(length(lens_ref, slot), beta)
        owner = slot >> 5
        n = jnp.where(owner == target, 0, n)
        i = slot & 31

        @pl.when(((owner >> 1) == chip) & (n > 0))
        def _():
            if other:
                start_copy(core, False, k_ref, v_ref, i * ROWS + start, stage, q, n, sem)
            else:
                row_copy(pre_ref, pre_at[i], stage, q, n, sem).start()

        @pl.when((owner >> 1) != chip)
        def _():
            from_links(plan, chip, slot, n, tables, TABLES * beta, recv, stage, q, sem)

        return q + n

    total = lax.fori_loop(0, SLOTS, one, I32(0))
    drain(stage, total, sem)
    flush(stage, 0, out_ref, total, sem)


def post_pack(beta, other, scalars, tables, k, v, pre, recv):
    recv = [recv[q // 3, q % 3] for q in range(9)]
    return local_call(
        functools.partial(post_kernel, beta, other),
        out_shape=rows_of(POST), out_specs=ANY,
        in_specs=[SMEM] * 9 + [ANY] * 12,
        scratch_shapes=[pltpu.VMEM((POST, KV, DIM), BF), pltpu.SMEM((SLOTS,), I32), pltpu.SemaphoreType.DMA],
    )(*scalars, *tables, k, v, pre, *recv)


ZEROS = 480


def zeros_kernel(dev_ref, lens_ref, src_ref, q_ref, ko_ref, vo_ref, lens_out, q_out, zeros, sem):
    dev = dev_ref[0]

    def clear(t, _):
        zeros[pl.ds(t * SLOTS, SLOTS)] = jnp.zeros((SLOTS, KV, DIM), BF)
        return 0

    lax.fori_loop(0, ZEROS // SLOTS, clear, 0)

    def each(wait, j, _):
        m = length(lens_ref, src_ref[dev * SLOTS + j])
        n = ROWS - 1 - m
        if not wait:
            lens_out[j] = m + 1

        @pl.when(n > 0)
        def _():
            for q, out in enumerate((ko_ref, vo_ref)):
                copy = row_copy(zeros, 0, out, j * ROWS + m + 1, n, sem.at[q, j])
                copy.wait() if wait else copy.start()

        return 0

    lax.fori_loop(0, SLOTS, functools.partial(each, False), 0)
    q_out[...] = q_ref[...]
    lax.fori_loop(0, SLOTS, functools.partial(each, True), 0)


def zero_tails(dev, lens, src, query):
    return local_call(
        zeros_kernel,
        out_shape=[rows_of(SLOTS * ROWS)] * 2 + [jax.ShapeDtypeStruct((SLOTS,), I32),
                                               jax.ShapeDtypeStruct(query.shape, BF)],
        out_specs=[ANY, ANY, SMEM, VMEM], in_specs=[SMEM] * 3 + [VMEM],
        scratch_shapes=[pltpu.VMEM((ZEROS, KV, DIM), BF), pltpu.SemaphoreType.DMA((2, SLOTS))],
    )(dev, lens, src, query)


N_BUF, AHEAD, UNROLL = 12, 8, 2


def finish_kernel(dev_ref, lens_ref, src_ref, k_ref, v_ref, *rest):
    land, post = rest[0:2], rest[2:4]
    q_ref, kn_ref, vn_ref, _, _, attn_ref, ko_ref, vo_ref, bufs, cols, moved_at, sem_in, sem_out = rest[4:]
    dev = dev_ref[0]
    core = dev & 1

    def source(j):
        slot = src_ref[dev * SLOTS + j]
        return slot, length(lens_ref, slot)

    def place(j, at):
        slot, m = source(j)
        after = []
        for beta in BATCHES:
            moved_at[SLOTS * beta + j] = at[beta]
            after.append(at[beta] + jnp.where((slot >> 5) != dev, part_of(m, beta)[1], 0))
        return tuple(after)

    lax.fori_loop(0, SLOTS, place, (I32(0), I32(0)))

    def fetch(j):
        slot, m = source(j)
        buf = lax.rem(j, N_BUF)

        @pl.when((slot >> 5) == dev)
        def _():
            home = (slot & 31) * ROWS
            row_copy(k_ref, home, bufs.at[0, buf], 0, m, sem_in.at[0, buf]).start()
            row_copy(v_ref, home, bufs.at[1, buf], 0, m, sem_in.at[1, buf]).start()

        @pl.when((slot >> 5) != dev)
        def _():
            for beta in BATCHES:
                start, n = part_of(m, beta)
                at = moved_at[SLOTS * beta + j]
                for ref, q in ((land[beta], core), (post[beta], 1 - core)):
                    row_copy(ref, at, bufs.at[q, buf], start, n, sem_in.at[q, buf]).start()

    def emit(j, wait):
        _, m = source(j)
        buf = lax.rem(j, N_BUF)
        for q, out in enumerate((ko_ref, vo_ref)):
            copy = row_copy(bufs.at[q, buf], 0, out, j * ROWS, m + 1, sem_out.at[q, buf])
            copy.wait() if wait else copy.start()

    def clear(t, _):
        bufs[1, t // KV, pl.ds((t % KV) * DIM, DIM)] = jnp.zeros((DIM, KV, DIM), BF)
        return 0

    lax.fori_loop(0, KV * N_BUF, clear, 0)

    def begin(j, _):
        fetch(j)
        return 0

    lax.fori_loop(0, AHEAD, begin, 0)
    head = lax.broadcasted_iota(I32, (HEADS, LANES), 0) // GROUP
    col = lax.broadcasted_iota(I32, (HEADS, LANES), 1)
    mine = jnp.where(head == (col & (KV - 1)), col, LAST // 2)

    def number(t, _):
        cols[:, pl.ds(pl.multiple_of(t * LANES, LANES), LANES)] = mine + t * LANES
        return 0

    lax.fori_loop(0, KV * ROWS // LANES, number, 0)

    def some(jj, _):
        def prefetch(u, _):
            ahead = UNROLL * jj + u + AHEAD

            @pl.when(ahead < SLOTS)
            def _():
                @pl.when(ahead >= N_BUF)
                def _():
                    emit(ahead - N_BUF, True)

                fetch(ahead)

            return 0

        lax.fori_loop(0, UNROLL, prefetch, 0)

        def ready(u, _):
            j = UNROLL * jj + u
            _, m = source(j)
            buf = lax.rem(j, N_BUF)
            for q, new in enumerate((kn_ref, vn_ref)):
                row_copy(k_ref, 0, bufs.at[q, buf], 0, m, sem_in.at[q, buf]).wait()
                bufs[q, buf, m] = new[j]
            emit(j, False)
            return 0

        lax.fori_loop(0, UNROLL, ready, 0)
        scores = []
        for u in range(UNROLL):
            j = UNROLL * jj + u
            kk = bufs[0, lax.rem(j, N_BUF)].reshape(KV * ROWS, DIM)
            s = lax.dot_general(q_ref[j], kk, (((1,), (1,)), ((), ())), preferred_element_type=F32)
            scores.append(jnp.where(cols[...] < KV * (source(j)[1] + 1), s * (DIM ** -0.5), -1e30))
        for u, s in enumerate(scores):
            j = UNROLL * jj + u
            p = jnp.exp(s - jnp.max(s, axis=1, keepdims=True))
            total = jnp.sum(p, axis=1, keepdims=True)
            vv = bufs[1, lax.rem(j, N_BUF)].reshape(KV * ROWS, DIM)
            acc = jnp.dot(p.astype(BF), vv, preferred_element_type=F32)
            attn_ref[j] = (acc / total).astype(BF)
        return 0

    lax.fori_loop(0, SLOTS // UNROLL, some, 0)

    def wait_out(j, _):
        emit(j, True)
        return 0

    lax.fori_loop(SLOTS - N_BUF, SLOTS, wait_out, 0)


def finish(scalars, k, v, land, post, query, k_new, v_new, outs):
    in_specs = [SMEM] * 3 + [ANY] * 6 + [VMEM] * 3
    dev, _, lens, _, src = scalars
    attn, ko, vo = local_call(
        finish_kernel,
        out_shape=[jax.ShapeDtypeStruct((SLOTS, HEADS, DIM), BF)] + [rows_of(SLOTS * ROWS)] * 2,
        out_specs=[VMEM, ANY, ANY], in_specs=in_specs + [ANY] * 2,
        input_output_aliases={len(in_specs): 1, len(in_specs) + 1: 2},
        scratch_shapes=[pltpu.VMEM((2, N_BUF, ROWS, KV, DIM), BF), pltpu.VMEM((HEADS, KV * ROWS), I32),
                        pltpu.SMEM((2 * SLOTS,), I32)] + [pltpu.SemaphoreType.DMA((2, N_BUF))] * 2,
    )(dev, lens, src, k, v, *land, *post, query, k_new, v_new, *outs)
    return attn, ko, vo


def swap(x, mask):
    return lax.ppermute(x, 'dp', [(i, i ^ mask) for i in range(DEVS)])


def after(x, *others):
    return lax.optimization_barrier((x, *others))[0]


def routed(rows, scalars, k, v, pre0, my_lens, query):
    dev, meta, lens, dest, src = scalars
    cap = caps_of(rows)
    recv, pre = [{}, {}], [pre0, None]
    turn = dev
    for step in range(3):
        for beta in BATCHES:
            if step == 0 and beta == 1:
                pre_send = pre_pack(1, False, turn, my_lens, dest, k, v)
                pre[1] = swap(pre_send, 1)
                ko, vo, lens_out, query = zero_tails(after(dev, pre_send), lens, src, query)
                tables = arrivals(after(dev, lens_out), meta)
                turn = after(dev, tables[0])
            sends = pack(beta, step, cap, (turn, *scalars[1:]), k, v, pre[beta], recv[beta])
            turn = after(dev, sends[0])
            for dim in range(3):
                recv[beta][step, dim] = swap(sends[dim], 2 << dim)
    land, post = [], []
    for beta in BATCHES:
        packed = post_pack(beta, True, (turn, *scalars[1:]), tables, k, v, pre[beta], recv[beta])
        turn = after(dev, packed)
        post.append(swap(packed, 1))
        land.append(post_pack(beta, False, (turn, *scalars[1:]), tables, k, v, pre[beta], recv[beta]))
        turn = after(dev, land[-1])
    return *land, *post, ko, vo, query, lens_out


def take_kernel(owner_ref, dev_ref, src_ref, kh, vh, _, __, ka, va, stage, sem):
    def one(j, _):
        slot = src_ref[dev_ref[0] * SLOTS + j]

        @pl.when((slot >> 5) == owner_ref[0])
        def _():
            for held, out in ((kh, ka), (vh, va)):
                row_copy(held, (slot & 31) * ROWS, stage, 0, ROWS, sem).start()
                row_copy(held, (slot & 31) * ROWS, stage, 0, ROWS, sem).wait()
                row_copy(stage, 0, out, j * ROWS, ROWS, sem).start()
                row_copy(stage, 0, out, j * ROWS, ROWS, sem).wait()

        return 0

    lax.fori_loop(0, SLOTS, one, 0)


def ring_move(dev, src, k, v):
    shift = [(i, (i + 1) % DEVS) for i in range(DEVS)]

    def turn(r, carry):
        owner = (dev - r) % DEVS
        ka, va = local_call(
            take_kernel, out_shape=[rows_of(SLOTS * ROWS)] * 2, out_specs=[ANY] * 2,
            in_specs=[SMEM] * 3 + [ANY] * 4, input_output_aliases={5: 0, 6: 1},
            scratch_shapes=[pltpu.VMEM((ROWS, KV, DIM), BF), pltpu.SemaphoreType.DMA],
        )(owner, dev, src, *carry)
        return *[lax.ppermute(x, 'dp', shift) for x in carry[:2]], ka, va

    first = turn(0, (k, v, jnp.zeros_like(k), jnp.zeros_like(v)))
    return lax.fori_loop(1, DEVS, turn, first)[2:]


def solution(mesh):
    def local(query, k_cache, v_cache, cache_lens, dest_slot, k_new, v_new):
        dev = lax.axis_index('dp').reshape(1).astype(I32)
        flat, full = (SLOTS * ROWS, KV, DIM), (SLOTS, ROWS, KV, DIM)
        k, v = k_cache.reshape(flat), v_cache.reshape(flat)
        lens = gather_lens(cache_lens)
        pre_send, src = pre_pack(0, True, after(dev, lens), cache_lens, dest_slot, k, v)
        pre0 = swap(pre_send, 1)
        plan = make_plan(lens, dest_slot)
        scalars = (dev, plan.reshape(-1), lens.reshape(-1), dest_slot, src)

        def route(rows, args):
            return routed(rows, *args)

        def fast(args):
            scalars, k, v, pre0, my_lens, query, k_new, v_new, pick = args
            branches = [functools.partial(route, rows) for rows in CLASSES]
            *came, ko, vo, query, lens_out = lax.switch(pick, branches, (scalars, k, v, pre0, my_lens, query))
            return *finish(scalars, k, v, came[:2], came[2:], query, k_new, v_new, (ko, vo)), lens_out

        def slow(args):
            (dev, meta, lens, dest, src), k, v, _, _, query, k_new, v_new, _ = args
            ka, va = ring_move(dev, src, k, v)
            mine = length(lens, lax.dynamic_slice(src, (dev[0] * SLOTS,), (SLOTS,)))
            mine = jnp.tile(jnp.pad(mine, (0, LANES - SLOTS)), DEVS)
            here = (dev, meta, mine, dest, jnp.arange(TOTAL, dtype=I32))
            none = [jnp.zeros((CHIPS, KV, DIM), BF)] * 2
            *outs, lens_out, query = zero_tails(dev, mine, here[-1], query)
            return *finish(here, ka, va, none, none, query, k_new, v_new, outs), lens_out

        pick = plan[C_ROW, 0]
        attn, ko, vo, lens_out = lax.cond(
            pick < len(CLASSES), fast, slow, (scalars, k, v, pre0, cache_lens, query, k_new, v_new, pick))
        return attn, ko.reshape(full), vo.reshape(full), lens_out

    row_spec = P('dp')
    return jax.shard_map(local, mesh=mesh, in_specs=(row_spec, row_spec, row_spec, row_spec, P(), row_spec, row_spec), out_specs=(row_spec, row_spec, row_spec, row_spec), check_vma=False)
```

```python
import functools
import itertools

import jax
import jax.numpy as jnp
import numpy as np
from jax import lax
from jax.experimental import pallas as pl
from jax.experimental.pallas import tpu as pltpu
from jax.sharding import PartitionSpec as P


I32, F32, BF = jnp.int32, jnp.float32, jnp.bfloat16
DEVS, SLOTS, TOTAL = 16, 32, 512
CHIPS, CHIP_SLOTS = 8, 64
DESTS = range(1, CHIPS)
ROWS = 256
HEADS, KV, TILE, DIM, GROUP = 28, 4, 8, 128, 7
PADDED = 32
LANES = 128
BATCHES = (0, 1)
PRE = 3456
POST = 3328
HALF = ROWS // 2
CLASSES = (1088, 1208, 1312, 1424, 1552, 1648, 1816, 2304)
ITERS, FIRST_STEP, SHRINK, MOMENTUM = 10, 0.675, 0.838, 0.9
LAST = jnp.iinfo(jnp.int32).max
VMEM_LIMIT = 62914560
TABLES = 40
LINKS = 3


def make_options():
    found = []
    for b in DESTS:
        dims = [k for k in range(LINKS) if (b >> k) & 1]
        mine = []
        for steps in itertools.combinations(range(3), len(dims)):
            for order in itertools.permutations(dims):
                place, hops = 0, []
                for step, k in zip(steps, order):
                    hops.append((step, place, k))
                    place ^= 1 << k
                mine.append((b, tuple(hops)))
        mine.sort(key=lambda option: (option[1][0][0], option[1][0][2], option[1]))
        found += mine
    return found


OPTIONS = make_options()
N_OPT = len(OPTIONS)
OPT_BASE = [next(o for o in range(N_OPT) if OPTIONS[o][0] == b) for b in DESTS]
OPT_COUNT = [sum(1 for x in OPTIONS if x[0] == b) for b in DESTS]


def make_flows():
    flows = {}
    for step in range(LINKS):
        for k in range(LINKS):
            runs = []
            for o, (_, hops) in enumerate(OPTIONS):
                for h, (st, place, kk) in enumerate(hops):
                    if (st, kk) == (step, k):
                        runs.append((place, o, h))
            runs.sort(key=lambda run: (run[0], run[1]))
            flows[step, k] = runs
    return flows


FLOWS = make_flows()
X_ROW, LO_ROW, S_ROW, C_ROW, META_ROWS = 0, 16, 32, 48, 56
PLACE_LANES = 16
BITS = (1, 2, 4)


def caps_of(rows):
    return rows // 2


def plan_consts():
    hop = np.zeros((LANES, LANES), np.float32)
    group = np.zeros_like(hop)
    before = np.zeros_like(hop)
    dest = np.zeros((CHIPS, LANES), np.float32)
    first = np.zeros_like(dest)
    for o, (b, hops) in enumerate(OPTIONS):
        dest[b, o] = 1
        first[:, o] = o == OPT_BASE[b - 1]
        for step, place, k in hops:
            hop[o, place * PLACE_LANES + step * 3 + k] = 1
        for q, (bb, _) in enumerate(OPTIONS):
            if bb == b:
                group[o, q] = 1
                before[o, q] = o < q
    tri = np.triu(np.ones_like(hop), 1)
    return hop, hop.T.copy(), group, before, dest, first, tri


def plan_kernel(lens_ref, dest_ref, hop_ref, hop_t_ref, group_ref, before_ref, dmat_ref, first_ref, tri_ref, out_ref):
    exact = functools.partial(jnp.dot, preferred_element_type=F32, precision=lax.Precision.HIGHEST)

    def plain(a, b):
        return jnp.dot(a.astype(BF), b.astype(BF), preferred_element_type=F32)

    shape = (CHIPS, LANES)
    row = lax.broadcasted_iota(I32, shape, 0)
    lane = lax.broadcasted_iota(I32, shape, 1)

    lens = lens_ref[...].reshape(CHIPS, 2 * LANES)
    lens = jnp.where(lane < SLOTS, lens[:, :LANES], pltpu.roll(lens[:, LANES:], SLOTS, 1))
    lens = jnp.where(lane < CHIP_SLOTS, (lens + 1) >> 1, 0)
    flat = dest_ref[...]
    turned = pltpu.roll(flat, CHIP_SLOTS, 1)
    to = jnp.concatenate([(turned if c & 1 else flat)[c >> 1:(c >> 1) + 1] for c in range(CHIPS)], axis=0)
    rel = (to >> 6) ^ row
    early = (lens + 1) >> 1
    parts = [early.astype(F32), (lens - early).astype(F32)]

    def top_of(a):
        return jnp.max(jnp.max(a, axis=1, keepdims=True), axis=0, keepdims=True)

    tri = tri_ref[...]
    dmat = dmat_ref[...]
    demand = []
    for beta in range(2):
        mine = [jnp.where(rel == b, parts[beta], 0.0) for b in DESTS]
        earlier = plain(jnp.concatenate(mine, axis=0), tri)
        starts = jnp.zeros(shape, F32)
        total = jnp.zeros(shape, F32)
        for b in DESTS:
            starts = jnp.where(rel == b, earlier[(b - 1) * CHIPS:b * CHIPS], starts)
            total = total + jnp.sum(mine[b - 1], axis=1, keepdims=True) * dmat[b:b + 1]
        demand.append(total)
        at = S_ROW + CHIPS * beta
        out_ref[at:at + CHIPS, :] = starts.astype(I32)

    def flip(a, bit):
        return jnp.where((row & bit) == 0, pltpu.roll(a, CHIPS - bit, 0), pltpu.roll(a, bit, 0))

    def link_loads(x, dot):
        y = dot(x, hop_ref[...])
        for bit in BITS[::-1]:
            y = y + flip(pltpu.roll(y, LANES - PLACE_LANES * bit, 1), bit)
            y = jnp.where(lane < PLACE_LANES * bit, y, 0.0)
        return y

    def path_cost(p):
        y = jnp.where(lane < PLACE_LANES, p, 0.0)
        for bit in BITS:
            y = y + pltpu.roll(flip(y, bit), PLACE_LANES * bit, 1)
        return plain(y, hop_t_ref[...])

    both = demand[0] + demand[1]
    used = jnp.sum(dmat, axis=0, keepdims=True) > 0

    def norm(w):
        w = jnp.where(used, jnp.maximum(w, 1e-6), 0.0)
        return w / jnp.where(used, plain(w, group_ref[...]), 1.0)

    weight = norm(jnp.ones(shape, F32))

    def improve(_, carry):
        weight, best, best_top, drift, size = carry
        loads = link_loads(weight * both, plain)
        top = top_of(loads)
        better = top < best_top
        best = jnp.where(better, weight, best)
        best_top = jnp.where(better, top, best_top)
        price = loads / jnp.maximum(top, 1.0)
        price = price * price
        cost = path_cost(price * price * price)
        drift = MOMENTUM * drift + cost
        weight = norm(weight * jnp.exp(-size * (MOMENTUM * drift + cost)))
        return weight, best, best_top, drift, size * SHRINK

    one = jnp.ones((1, 1), F32)
    start = (weight, weight, 3e38 * one, jnp.zeros(shape, F32), FIRST_STEP * one)
    best = lax.fori_loop(0, ITERS, improve, start)[1]

    pick = jnp.zeros((1, 1), I32)
    for t in range(2):
        total = demand[t]
        x = jnp.minimum(jnp.floor(best * total * 0.995), total)
        x = x + first_ref[...] * (total - exact(x, group_ref[...]))
        top = top_of(link_loads(x, exact))
        top = jnp.where(top_of(-x) > 0.0, 1e6, top)
        need = jnp.zeros((1, 1), I32)
        for rows in CLASSES:
            need = need + (top > caps_of(rows)).astype(I32)
        pick = jnp.maximum(pick, need)
        at = X_ROW + CHIPS * t
        out_ref[at:at + CHIPS, :] = x.astype(I32)
        at = LO_ROW + CHIPS * t
        out_ref[at:at + CHIPS, :] = exact(x, before_ref[...]).astype(I32)

    from_dev = 2 * row + (lane >> 5)
    to_dev = to >> 5
    crossing = jnp.where(from_dev == to_dev, 0.0, parts[0])
    come = jnp.concatenate([jnp.where(to_dev == d, crossing, 0.0) for d in range(DEVS)], axis=0)
    come = plain(come, jnp.ones((LANES, LANES), F32)).reshape(DEVS, CHIPS, LANES)
    over = top_of(jnp.sum(come, axis=1)) - POST
    for core in range(2):
        leave = jnp.where((lane >> 5) == core, crossing, 0.0)
        over = jnp.maximum(over, top_of(jnp.sum(leave, axis=1, keepdims=True)) - PRE)
    pick = jnp.where(over > 0.0, len(CLASSES), pick)
    out_ref[C_ROW:C_ROW + CHIPS, :] = jnp.broadcast_to(pick, shape)


def make_plan(lens_all, dest_slot):
    return pl.pallas_call(
        plan_kernel,
        out_shape=jax.ShapeDtypeStruct((META_ROWS, LANES), I32),
        name='plan',
    )(lens_all, dest_slot.reshape(KV, LANES), *plan_consts())


def gather_kernel(x_ref, out_ref, send_sem, recv_sem):
    me = lax.axis_index('dp')
    barrier = pltpu.get_barrier_semaphore()
    for r in range(1, DEVS):
        pl.semaphore_signal(barrier, inc=1, device_id=(lax.rem(me + r, DEVS),), device_id_type=pl.DeviceIdType.MESH)
    pl.semaphore_wait(barrier, DEVS - 1)
    copies = []
    for r in range(1, DEVS):
        copies.append(pltpu.make_async_remote_copy(
            src_ref=x_ref, dst_ref=out_ref.at[me], send_sem=send_sem.at[r], recv_sem=recv_sem.at[r],
            device_id=(lax.rem(me + r, DEVS),), device_id_type=pl.DeviceIdType.MESH))
        copies[-1].start()
    out_ref[me] = x_ref[...]
    for copy in copies:
        copy.wait()


def gather_lens(my_lens):
    row = jnp.pad(my_lens, (0, LANES - SLOTS)).reshape(1, LANES)
    return pl.pallas_call(
        gather_kernel,
        out_shape=jax.ShapeDtypeStruct((DEVS, 1, LANES), I32),
        in_specs=[VMEM], out_specs=VMEM,
        scratch_shapes=[pltpu.SemaphoreType.DMA((DEVS,))] * 2,
        compiler_params=pltpu.CompilerParams(collective_id=0, has_side_effects=True),
        name='gather_lens',
    )(row).reshape(DEVS, LANES)


def length(lens_ref, slot):
    return lens_ref[(slot >> 5) * LANES + (slot & 31)]


def pairs_of(m):
    return (m + 1) >> 1


def part_of(m, beta):
    early = (m + 3) >> 2
    return (0, early)[beta], (early, pairs_of(m) - early)[beta]


def row_copy(src, s0, dst, d0, n, sem):
    return pltpu.make_async_copy(src.at[pl.ds(s0, n)], dst.at[pl.ds(d0, n)], sem)


def drain(ref, n, sem):
    @pl.when(n > 0)
    def _():
        row_copy(ref, 0, ref, 0, n, sem).wait()


def flush(stage, s0, out, n, sem):
    @pl.when(n > 0)
    def _():
        copy = row_copy(stage, s0, out, 0, n, sem)
        copy.start()
        copy.wait()


def start_copy(core, flip, k_ref, v_ref, s0, dst, d0, n, sem):
    for c, ref in enumerate((v_ref, k_ref) if flip else (k_ref, v_ref)):
        @pl.when(core == c)
        def _(ref=ref):
            row_copy(ref, s0, dst, d0, n, sem).start()


SMEM = pl.BlockSpec(memory_space=pltpu.SMEM)
ANY = pl.BlockSpec(memory_space=pltpu.HBM)
VMEM = pl.BlockSpec(memory_space=pltpu.VMEM)


def rows_of(n, dtype=BF):
    return jax.ShapeDtypeStruct((n, TILE, DIM), dtype)


def local_call(kernel, **kwargs):
    return pl.pallas_call(
        kernel, compiler_params=pltpu.CompilerParams(vmem_limit_bytes=VMEM_LIMIT), **kwargs)


def pre_kernel(beta, with_src, dev_ref, lens_ref, dest_ref, k_ref, v_ref, out_ref, *rest):
    if with_src:
        src_ref, stage, sem = rest
    else:
        stage, sem = rest
    dev = dev_ref[0]
    core = dev & 1

    def one(i, q):
        start, n = part_of(lens_ref[i], beta)
        moving = (dest_ref[dev * SLOTS + i] >> 5) != dev
        n = jnp.where(moving, n, 0)

        @pl.when(n > 0)
        def _():
            start_copy(core, True, k_ref, v_ref, i * ROWS + start, stage, q, n, sem)

        return q + n

    total = lax.fori_loop(0, SLOTS, one, I32(0))
    if with_src:
        def invert(i, _):
            for u in range(CHIPS):
                at = i * CHIPS + u
                src_ref[dest_ref[at]] = at
            return 0

        lax.fori_loop(0, TOTAL // CHIPS, invert, 0)
    drain(stage, total, sem)
    flush(stage, 0, out_ref, jnp.minimum(total, PRE), sem)


def pre_pack(beta, with_src, dev, lens, dest, k, v):
    out, specs = [rows_of(PRE)], [ANY]
    if with_src:
        out.append(jax.ShapeDtypeStruct((TOTAL,), I32))
        specs.append(SMEM)
    got = local_call(
        functools.partial(pre_kernel, beta, with_src),
        out_shape=out, out_specs=specs, in_specs=[SMEM] * 3 + [ANY] * 2,
        scratch_shapes=[pltpu.VMEM((SLOTS * HALF, TILE, DIM), BF), pltpu.SemaphoreType.DMA],
    )(dev, lens, dest, k, v)
    return got if with_src else got[0]


class Table:
    def __init__(self, meta, chip, beta):
        self.meta, self.at = meta, CHIPS * BATCHES[beta]
        self.row = [(self.at + (chip ^ v)) * LANES for v in range(CHIPS)]

    def x(self, v, o):
        return self.meta[X_ROW * LANES + self.row[v] + o]

    def lo(self, v, o):
        return self.meta[LO_ROW * LANES + self.row[v] + o]

    def start(self, slot):
        return self.meta[S_ROW * LANES + (self.at + (slot // CHIP_SLOTS)) * LANES + (slot & 63)]


def pack_kernel(beta, step, cap, dev_ref, meta, lens_ref, dest_ref, k_ref, v_ref, pre_ref, *rest):
    recv = {}
    n_in = 3 * step
    for q in range(n_in):
        recv[q // 3, q % 3] = rest[q]
    outs = rest[n_in:n_in + 3]
    stage, table_lo, table_hi, table_to, sem, sem_out = rest[n_in + 3:]
    dev = dev_ref[0]
    chip, core = dev >> 1, dev & 1
    plan = Table(meta, chip, beta)
    used = []
    count = I32(0)
    for k in range(LINKS):
        where = I32(0)
        spans = {}
        for place, o, _ in FLOWS[step, k]:
            if place == 0:
                b = OPTIONS[o][0]
                n = plan.x(0, o)
                if b not in spans:
                    spans[b] = [plan.lo(0, o), I32(0), where]
                spans[b][1] = spans[b][1] + n
                where = where + n
        for b in DESTS:
            if b in spans:
                lo, n, to = spans[b]
                table_lo[b * 3 + k] = lo
                table_hi[b * 3 + k] = lo + n
                table_to[b * 3 + k] = to - lo + k * cap
            else:
                table_lo[b * 3 + k] = I32(0)
                table_hi[b * 3 + k] = I32(0)
                table_to[b * 3 + k] = I32(0)
        used.append(where)
        count = count + where

    if step > 0:
        came = {}
        for (st, kk), runs in FLOWS.items():
            if st < step:
                at = I32(0)
                for place, o, h in runs:
                    v = place ^ (1 << kk)
                    n = plan.x(v, o)
                    hops = OPTIONS[o][1]
                    if h + 1 < len(hops) and hops[h + 1][0] == step:
                        came[v, o] = (st, kk, at, n)
                    at = at + n
        for k in range(LINKS):
            for place, o, h in FLOWS[step, k]:
                if place == 0:
                    continue
                st, kk, at, n = came[place, o]

                @pl.when(n > 0)
                def _(st=st, kk=kk, at=at, n=n, to=used[k], k=k):
                    row_copy(recv[st, kk], at, stage, to + k * cap, n, sem).start()

                used[k] = used[k] + n
                count = count + n

    def one(i, q):
        slot = chip * 64 + i
        to_slot = dest_ref[slot]
        mine = (i >> 5) == core
        start, n = part_of(length(lens_ref, slot), beta)
        b = chip ^ (to_slot >> 6)

        @pl.when(b > 0)
        def _():
            begin = plan.start(slot)
            for k in range(LINKS):
                lo = jnp.maximum(begin, table_lo[b * 3 + k])
                hi = jnp.minimum(begin + n, table_hi[b * 3 + k])
                size = hi - lo
                to = table_to[b * 3 + k] + lo
                skip = lo - begin

                @pl.when(size > 0)
                def _():
                    home = (i & 31) * ROWS + start + skip

                    @pl.when(mine)
                    def _():
                        start_copy(core, False, k_ref, v_ref, home, stage, to, size, sem)

                    @pl.when(jnp.logical_not(mine))
                    def _():
                        row_copy(pre_ref, q + skip, stage, to, size, sem).start()

        away = jnp.logical_not(mine) & ((to_slot >> 5) != (slot >> 5))
        return q + jnp.where(away, n, 0)

    lax.fori_loop(0, 64, one, I32(0))
    drain(stage, count, sem)
    for k in range(LINKS):
        @pl.when(used[k] > 0)
        def _(k=k):
            row_copy(stage, k * cap, outs[k], 0, used[k], sem_out.at[k]).start()
    for k in range(LINKS):
        @pl.when(used[k] > 0)
        def _(k=k):
            row_copy(stage, k * cap, outs[k], 0, used[k], sem_out.at[k]).wait()


def pack(beta, step, cap, scalars, k, v, pre, recv):
    dev, meta, lens, dest, _ = scalars
    recv = [recv[q // 3, q % 3] for q in range(3 * step)]
    return local_call(
        functools.partial(pack_kernel, beta, step, cap),
        out_shape=[rows_of(cap)] * 3, out_specs=[ANY] * 3,
        in_specs=[SMEM] * 4 + [ANY] * (3 + len(recv)),
        scratch_shapes=[pltpu.VMEM((3 * cap, TILE, DIM), BF)] + [pltpu.SMEM((TABLES,), I32)] * 3
        + [pltpu.SemaphoreType.DMA, pltpu.SemaphoreType.DMA((3,))],
    )(dev, meta, lens, dest, k, v, pre, *recv)


def table_kernel(dev_ref, meta, lo_ref, hi_ref, at_ref, buf_ref):
    for beta in BATCHES:
        plan = Table(meta, dev_ref[0] >> 1, beta)
        base = TABLES * beta
        for (st, kk), runs in FLOWS.items():
            at = I32(0)
            for place, o, h in runs:
                v = place ^ (1 << kk)
                n = plan.x(v, o)
                if h + 1 == len(OPTIONS[o][1]):
                    lo = plan.lo(v, o)
                    lo_ref[base + o] = lo
                    hi_ref[base + o] = lo + n
                    at_ref[base + o] = at - lo
                    buf_ref[base + o] = I32(st * 3 + kk)
                at = at + n


def arrivals(dev, meta):
    return local_call(
        table_kernel, out_shape=[jax.ShapeDtypeStruct((2 * TABLES,), I32)] * 4,
        out_specs=[SMEM] * 4, in_specs=[SMEM] * 2)(dev, meta)


def static_lookup(table, index):
    out = I32(table[0])
    for q in range(1, len(table)):
        out = jnp.where(index == q, I32(table[q]), out)
    return out


def from_links(plan, chip, slot, n, tables, base, recv, dst, to, sem):
    table_lo, table_hi, table_at, buf_ref = tables
    b = chip ^ (slot // CHIP_SLOTS)
    begin = plan.start(slot)
    first = static_lookup([0] + OPT_BASE, b)
    count = static_lookup([0] + OPT_COUNT, b)

    def piece(q, _):
        o = first + q
        lo = jnp.maximum(begin, table_lo[base + o])
        hi = jnp.minimum(begin + n, table_hi[base + o])
        size = hi - lo
        at = table_at[base + o] + lo
        put = to + lo - begin

        @pl.when(size > 0)
        def _():
            which = buf_ref[base + o]
            for w in range(9):
                @pl.when(which == w)
                def _(w=w):
                    row_copy(recv[w], at, dst, put, size, sem).start()

        return 0

    lax.fori_loop(0, count, piece, 0)


def post_kernel(beta, other, dev_ref, meta, lens_ref, dest_ref, src_ref, *rest):
    tables, (k_ref, v_ref, pre_ref, *recv), rest = rest[:4], rest[4:16], rest[16:]
    if other:
        out_ref, stage, sem = rest
    else:
        ko_ref, vo_ref, stage, pre_at, sem, sem_out = rest[2:]
    dev = dev_ref[0]
    chip, core = dev >> 1, dev & 1
    plan = Table(meta, chip, beta)
    sibling = dev ^ 1
    target = sibling if other else dev

    if not other:
        def place(i, q):
            pre_at[i] = q
            slot = sibling * SLOTS + i
            _, n = part_of(length(lens_ref, slot), beta)
            return q + jnp.where((dest_ref[slot] >> 5) != sibling, n, 0)

        lax.fori_loop(0, SLOTS, place, I32(0))

    def one(j, q):
        slot = src_ref[target * SLOTS + j]
        start, n = part_of(length(lens_ref, slot), beta)
        owner = slot >> 5
        n = jnp.where(owner == target, 0, n)
        i = slot & 31

        @pl.when(((owner >> 1) == chip) & (n > 0))
        def _():
            if other:
                start_copy(core, False, k_ref, v_ref, i * ROWS + start, stage, q, n, sem)
            else:
                row_copy(pre_ref, pre_at[i], stage, q, n, sem).start()

        @pl.when((owner >> 1) != chip)
        def _():
            from_links(plan, chip, slot, n, tables, TABLES * beta, recv, stage, q, sem)

        return q + n

    total = lax.fori_loop(0, SLOTS, one, I32(0))
    drain(stage, total, sem)
    if other:
        flush(stage, 0, out_ref, total, sem)
        return

    def put(j, q):
        slot = src_ref[target * SLOTS + j]
        start, n = part_of(length(lens_ref, slot), beta)
        n = jnp.where((slot >> 5) == target, 0, n)

        @pl.when(n > 0)
        def _():
            for c, out in enumerate((ko_ref, vo_ref)):
                @pl.when(core == c)
                def _(out=out):
                    row_copy(stage, q, out, j * ROWS + start, n, sem_out).start()

        return q + n

    lax.fori_loop(0, SLOTS, put, I32(0))
    drain(stage, total, sem_out)


def post_pack(beta, scalars, tables, k, v, pre, recv):
    return local_call(
        functools.partial(post_kernel, beta, True),
        out_shape=rows_of(POST), out_specs=ANY,
        in_specs=[SMEM] * 9 + [ANY] * 12,
        scratch_shapes=[pltpu.VMEM((POST, TILE, DIM), BF), pltpu.SemaphoreType.DMA],
    )(*scalars, *tables, k, v, pre, *[recv[q // LINKS, q % LINKS] for q in range(LINKS * LINKS)])


def land(beta, scalars, tables, k, v, pre, recv, outs):
    in_specs = [SMEM] * 9 + [ANY] * 12
    return local_call(
        functools.partial(post_kernel, beta, False),
        out_shape=[rows_of(SLOTS * ROWS)] * 2, out_specs=[ANY] * 2, in_specs=in_specs + [ANY] * 2,
        input_output_aliases={len(in_specs): 0, len(in_specs) + 1: 1},
        scratch_shapes=[pltpu.VMEM((POST, TILE, DIM), BF), pltpu.SMEM((SLOTS,), I32)] + [pltpu.SemaphoreType.DMA] * 2,
    )(*scalars, *tables, k, v, pre, *[recv[q // LINKS, q % LINKS] for q in range(LINKS * LINKS)], *outs)


ZEROS = 256


def zeros_kernel(dev_ref, lens_ref, src_ref, q_ref, ko_ref, vo_ref, lens_out, q_out, zeros, sem):
    dev = dev_ref[0]

    def clear(t, _):
        zeros[pl.ds(t * SLOTS, SLOTS)] = jnp.zeros((SLOTS, TILE, DIM), BF)
        return 0

    lax.fori_loop(0, ZEROS // SLOTS, clear, 0)

    def each(wait, j, _):
        m = length(lens_ref, src_ref[dev * SLOTS + j])
        behind = (m >> 1) + 1
        n = ROWS - behind
        if not wait:
            lens_out[j] = m + 1

        @pl.when(n > 0)
        def _():
            for q, out in enumerate((ko_ref, vo_ref)):
                copy = row_copy(zeros, 0, out, j * ROWS + behind, n, sem.at[q, j])
                copy.wait() if wait else copy.start()

        return 0

    lax.fori_loop(0, SLOTS, functools.partial(each, False), 0)
    q_out[...] = jnp.zeros_like(q_out)
    q_out[:, :HEADS] = q_ref[...]
    lax.fori_loop(0, SLOTS, functools.partial(each, True), 0)


def zero_tails(dev, lens, src, query):
    return local_call(
        zeros_kernel,
        out_shape=[rows_of(SLOTS * ROWS)] * 2 + [jax.ShapeDtypeStruct((SLOTS,), I32),
                                               jax.ShapeDtypeStruct((SLOTS, PADDED, DIM), BF)],
        out_specs=[ANY, ANY, SMEM, VMEM], in_specs=[SMEM] * 3 + [VMEM],
        scratch_shapes=[pltpu.VMEM((ZEROS, TILE, DIM), BF), pltpu.SemaphoreType.DMA((2, SLOTS))],
    )(dev, lens, src, query)


N_BUF, AHEAD, UNROLL = 12, 8, 4


def finish_kernel(dev_ref, lens_ref, src_ref, k_ref, v_ref, *rest):
    post = rest[0:2]
    q_ref, kn_ref, vn_ref, _, _, attn_ref, ko_ref, vo_ref, bufs, cols, moved_at, sem_in, sem_out = rest[2:]
    dev = dev_ref[0]
    core = dev & 1

    def source(j):
        slot = src_ref[dev * SLOTS + j]
        return slot, length(lens_ref, slot)

    def place(j, at):
        slot, m = source(j)
        after = []
        for beta in BATCHES:
            moved_at[SLOTS * beta + j] = at[beta]
            after.append(at[beta] + jnp.where((slot >> 5) != dev, part_of(m, beta)[1], 0))
        return tuple(after)

    lax.fori_loop(0, SLOTS, place, (I32(0), I32(0)))

    def fetch(j):
        slot, m = source(j)
        buf = lax.rem(j, N_BUF)

        @pl.when((slot >> 5) == dev)
        def _():
            home = (slot & 31) * ROWS
            row_copy(k_ref, home, bufs.at[0, buf], 0, pairs_of(m), sem_in.at[0, buf]).start()
            row_copy(v_ref, home, bufs.at[1, buf], 0, pairs_of(m), sem_in.at[1, buf]).start()

        @pl.when((slot >> 5) != dev)
        def _():
            start_copy(core, False, ko_ref, vo_ref, j * ROWS, bufs.at[core, buf], 0, pairs_of(m), sem_in.at[core, buf])
            for beta in BATCHES:
                start, n = part_of(m, beta)
                row_copy(post[beta], moved_at[SLOTS * beta + j], bufs.at[1 - core, buf], start, n,
                         sem_in.at[1 - core, buf]).start()

    def emit(j, wait):
        slot, m = source(j)
        buf = lax.rem(j, N_BUF)
        for q, out in enumerate((ko_ref, vo_ref)):
            here = ((slot >> 5) != dev) & (core == q)
            end = m >> 1
            first = jnp.where(here, end, 0)
            copy = row_copy(bufs.at[q, buf], first, out, j * ROWS + first, end + 1 - first, sem_out.at[q, buf])
            copy.wait() if wait else copy.start()

    def clear(t, _):
        bufs[1, t // 2, pl.ds((t % 2) * DIM, DIM)] = jnp.zeros((DIM, TILE, DIM), BF)
        return 0

    lax.fori_loop(0, 2 * N_BUF, clear, 0)

    def begin(j, _):
        fetch(j)
        return 0

    lax.fori_loop(0, AHEAD, begin, 0)
    half = lax.broadcasted_iota(I32, (TILE, DIM), 0) // KV
    head = lax.broadcasted_iota(I32, (PADDED, LANES), 0) // GROUP
    col = lax.broadcasted_iota(I32, (PADDED, LANES), 1)
    mine = jnp.where(head == (col & (KV - 1)), col, LAST // 2)

    def number(t, _):
        cols[:, pl.ds(pl.multiple_of(t * LANES, LANES), LANES)] = mine + t * LANES
        return 0

    lax.fori_loop(0, TILE * ROWS // LANES, number, 0)

    def some(jj, _):
        def prefetch(u, _):
            ahead = UNROLL * jj + u + AHEAD

            @pl.when(ahead < SLOTS)
            def _():
                @pl.when(ahead >= N_BUF)
                def _():
                    emit(ahead - N_BUF, True)

                fetch(ahead)

            return 0

        lax.fori_loop(0, UNROLL, prefetch, 0)

        def ready(u, _):
            j = UNROLL * jj + u
            _, m = source(j)
            buf = lax.rem(j, N_BUF)
            for q, new in enumerate((kn_ref, vn_ref)):
                row_copy(k_ref, 0, bufs.at[q, buf], 0, pairs_of(m), sem_in.at[q, buf]).wait()
                both = jnp.concatenate([new[j], new[j]], axis=0)
                kept = jnp.where(half < (m & 1), bufs[q, buf, m >> 1], jnp.zeros_like(both))
                bufs[q, buf, m >> 1] = jnp.where(half == (m & 1), both, kept)
            emit(j, False)
            return 0

        lax.fori_loop(0, UNROLL, ready, 0)
        scores = []
        for u in range(UNROLL):
            j = UNROLL * jj + u
            kk = bufs[0, lax.rem(j, N_BUF)].reshape(TILE * ROWS, DIM)
            s = lax.dot_general(q_ref[j], kk, (((1,), (1,)), ((), ())), preferred_element_type=F32)
            scores.append(jnp.where(cols[...] < KV * (source(j)[1] + 1), s * (DIM ** -0.5), -1e30))
        for u, s in enumerate(scores):
            j = UNROLL * jj + u
            p = jnp.exp(s - jnp.max(s, axis=1, keepdims=True))
            total = jnp.sum(p, axis=1, keepdims=True)
            vv = bufs[1, lax.rem(j, N_BUF)].reshape(TILE * ROWS, DIM)
            acc = jnp.dot(p.astype(BF), vv, preferred_element_type=F32)
            attn_ref[j] = (acc / total)[:HEADS].astype(BF)
        return 0

    lax.fori_loop(0, SLOTS // UNROLL, some, 0)

    def wait_out(j, _):
        emit(j, True)
        return 0

    lax.fori_loop(SLOTS - N_BUF, SLOTS, wait_out, 0)


def finish(scalars, k, v, post, query, k_new, v_new, outs):
    in_specs = [SMEM] * 3 + [ANY] * 4 + [VMEM] * 3
    dev, _, lens, _, src = scalars
    attn, ko, vo = local_call(
        finish_kernel,
        out_shape=[jax.ShapeDtypeStruct((SLOTS, HEADS, DIM), BF)] + [rows_of(SLOTS * ROWS)] * 2,
        out_specs=[VMEM, ANY, ANY], in_specs=in_specs + [ANY] * 2,
        input_output_aliases={len(in_specs): 1, len(in_specs) + 1: 2},
        scratch_shapes=[pltpu.VMEM((2, N_BUF, ROWS, TILE, DIM), BF), pltpu.VMEM((PADDED, TILE * ROWS), I32),
                        pltpu.SMEM((2 * SLOTS,), I32)] + [pltpu.SemaphoreType.DMA((2, N_BUF))] * 2,
    )(dev, lens, src, k, v, *post, query, k_new, v_new, *outs)
    return attn, ko, vo


def swap(x, mask):
    return lax.ppermute(x, 'dp', [(i, i ^ mask) for i in range(DEVS)])


def after(x, *others):
    return lax.optimization_barrier((x, *others))[0]


def routed(rows, scalars, k, v, pre0, my_lens, query):
    dev, meta, lens, dest, src = scalars
    cap = caps_of(rows)
    recv, pre = [{}, {}], [pre0, None]
    turn = dev
    for step in range(LINKS):
        for beta in BATCHES:
            if step == 0 and beta == 1:
                pre_send = pre_pack(1, False, turn, my_lens, dest, k, v)
                pre[1] = swap(pre_send, 1)
                ko, vo, lens_out, query = zero_tails(after(dev, pre_send), lens, src, query)
                tables = arrivals(after(dev, lens_out), meta)
                turn = after(dev, tables[0])
            sends = pack(beta, step, cap, (turn, *scalars[1:]), k, v, pre[beta], recv[beta])
            turn = after(dev, sends[0])
            for dim in range(LINKS):
                recv[beta][step, dim] = swap(sends[dim], 2 << dim)
    post, outs = [], (ko, vo)
    for beta in BATCHES:
        packed = post_pack(beta, (turn, *scalars[1:]), tables, k, v, pre[beta], recv[beta])
        turn = after(dev, packed)
        post.append(swap(packed, 1))
        outs = land(beta, (turn, *scalars[1:]), tables, k, v, pre[beta], recv[beta], outs)
        turn = after(dev, outs[0])
    return *post, *outs, query, lens_out


def take_kernel(owner_ref, dev_ref, src_ref, kh, vh, _, __, ka, va, stage, sem):
    def one(j, _):
        slot = src_ref[dev_ref[0] * SLOTS + j]

        @pl.when((slot >> 5) == owner_ref[0])
        def _():
            for held, out in ((kh, ka), (vh, va)):
                row_copy(held, (slot & 31) * ROWS, stage, 0, ROWS, sem).start()
                row_copy(held, (slot & 31) * ROWS, stage, 0, ROWS, sem).wait()
                row_copy(stage, 0, out, j * ROWS, ROWS, sem).start()
                row_copy(stage, 0, out, j * ROWS, ROWS, sem).wait()

        return 0

    lax.fori_loop(0, SLOTS, one, 0)


def ring_move(dev, src, k, v):
    shift = [(i, (i + 1) % DEVS) for i in range(DEVS)]

    def turn(r, carry):
        owner = (dev - r) % DEVS
        ka, va = local_call(
            take_kernel, out_shape=[rows_of(SLOTS * ROWS)] * 2, out_specs=[ANY] * 2,
            in_specs=[SMEM] * 3 + [ANY] * 4, input_output_aliases={5: 0, 6: 1},
            scratch_shapes=[pltpu.VMEM((ROWS, TILE, DIM), BF), pltpu.SemaphoreType.DMA],
        )(owner, dev, src, *carry)
        return *[lax.ppermute(x, 'dp', shift) for x in carry[:2]], ka, va

    first = turn(0, (k, v, jnp.zeros_like(k), jnp.zeros_like(v)))
    return lax.fori_loop(1, DEVS, turn, first)[2:]


def solution(mesh):
    def local(query, k_cache, v_cache, cache_lens, dest_slot, k_new, v_new):
        dev = lax.axis_index('dp').reshape(1).astype(I32)
        flat, full = (SLOTS * ROWS, TILE, DIM), k_cache.shape
        k, v = k_cache.reshape(flat), v_cache.reshape(flat)
        lens = gather_lens(cache_lens)
        pre_send, src = pre_pack(0, True, after(dev, lens), cache_lens, dest_slot, k, v)
        pre0 = swap(pre_send, 1)
        plan = make_plan(lens, dest_slot)
        scalars = (dev, plan.reshape(-1), lens.reshape(-1), dest_slot, src)

        def route(rows, args):
            return routed(rows, *args)

        def fast(args):
            scalars, k, v, pre0, my_lens, query, k_new, v_new, pick = args
            branches = [functools.partial(route, rows) for rows in CLASSES]
            *post, ko, vo, query, lens_out = lax.switch(pick, branches, (scalars, k, v, pre0, my_lens, query))
            return *finish(scalars, k, v, post, query, k_new, v_new, (ko, vo)), lens_out

        def slow(args):
            (dev, meta, lens, dest, src), k, v, _, _, query, k_new, v_new, _ = args
            ka, va = ring_move(dev, src, k, v)
            mine = length(lens, lax.dynamic_slice(src, (dev[0] * SLOTS,), (SLOTS,)))
            mine = jnp.tile(jnp.pad(mine, (0, LANES - SLOTS)), DEVS)
            here = (dev, meta, mine, dest, jnp.arange(TOTAL, dtype=I32))
            none = [jnp.zeros((CHIPS, TILE, DIM), BF)] * 2
            *outs, lens_out, query = zero_tails(dev, mine, here[-1], query)
            return *finish(here, ka, va, none, query, k_new, v_new, outs), lens_out

        pick = plan[C_ROW, 0]
        attn, ko, vo, lens_out = lax.cond(
            pick < len(CLASSES), fast, slow, (scalars, k, v, pre0, cache_lens, query, k_new, v_new, pick))
        return attn, ko.reshape(full), vo.reshape(full), lens_out

    row_spec = P('dp')
    return jax.shard_map(local, mesh=mesh, in_specs=(row_spec, row_spec, row_spec, row_spec, P(), row_spec, row_spec), out_specs=(row_spec, row_spec, row_spec, row_spec), check_vma=False)
```

```python
import functools
import itertools

import jax
import jax.numpy as jnp
import numpy as np
from jax import lax
from jax.experimental import pallas as pl
from jax.experimental.pallas import tpu as pltpu
from jax.sharding import PartitionSpec as P


I32, F32, BF = jnp.int32, jnp.float32, jnp.bfloat16
DEVS, SLOTS, TOTAL = 16, 32, 512
CHIPS, CHIP_SLOTS = 8, 64
DESTS = range(1, CHIPS)
ROWS = 256
HEADS, KV, TILE, DIM, GROUP = 28, 4, 8, 128, 7
PADDED = 32
LANES = 128
BATCHES = (0, 1)
PRE = 3456
POST = 3328
HALF = ROWS // 2
CLASSES = (1080, 1200, 1304, 1408, 1528, 1648, 1840, 2400)
ITERS, FIRST_STEP, SHRINK, MOMENTUM = 10, 0.675, 0.838, 0.9
LAST = jnp.iinfo(jnp.int32).max
VMEM_LIMIT = 62914560
TABLES = 40
LINKS = 3


def make_options():
    found = []
    for b in DESTS:
        dims = [k for k in range(LINKS) if (b >> k) & 1]
        mine = []
        for steps in itertools.combinations(range(3), len(dims)):
            for order in itertools.permutations(dims):
                place, hops = 0, []
                for step, k in zip(steps, order):
                    hops.append((step, place, k))
                    place ^= 1 << k
                mine.append((b, tuple(hops)))
        mine.sort(key=lambda option: (option[1][0][0], option[1][0][2], option[1]))
        found += mine
    return found


OPTIONS = make_options()
N_OPT = len(OPTIONS)
OPT_BASE = [next(o for o in range(N_OPT) if OPTIONS[o][0] == b) for b in DESTS]
OPT_COUNT = [sum(1 for x in OPTIONS if x[0] == b) for b in DESTS]


def make_flows():
    flows = {}
    for step in range(LINKS):
        for k in range(LINKS):
            runs = []
            for o, (_, hops) in enumerate(OPTIONS):
                for h, (st, place, kk) in enumerate(hops):
                    if (st, kk) == (step, k):
                        runs.append((place, o, h))
            runs.sort(key=lambda run: (run[0], run[1]))
            flows[step, k] = runs
    return flows


FLOWS = make_flows()
X_ROW, LO_ROW, S_ROW, C_ROW, META_ROWS = 0, 16, 32, 48, 56
PLACE_LANES = 16
BITS = (1, 2, 4)


def caps_of(rows):
    return rows // 2


def plan_consts():
    hop = np.zeros((LANES, LANES), np.float32)
    group = np.zeros_like(hop)
    before = np.zeros_like(hop)
    dest = np.zeros((CHIPS, LANES), np.float32)
    last = np.zeros_like(dest)
    for o, (b, hops) in enumerate(OPTIONS):
        dest[b, o] = 1
        last[:, o] = o == OPT_BASE[b - 1] + OPT_COUNT[b - 1] - 1
        for step, place, k in hops:
            hop[o, place * PLACE_LANES + step * 3 + k] = 1
        for q, (bb, _) in enumerate(OPTIONS):
            if bb == b:
                group[o, q] = 1
                before[o, q] = o < q
    tri = np.triu(np.ones_like(hop), 1)
    return hop, hop.T.copy(), group, before, dest, last, tri


def plan_kernel(lens_ref, dest_ref, hop_ref, hop_t_ref, group_ref, before_ref, dmat_ref, last_ref, tri_ref, out_ref):
    exact = functools.partial(jnp.dot, preferred_element_type=F32, precision=lax.Precision.HIGHEST)

    def plain(a, b):
        return jnp.dot(a.astype(BF), b.astype(BF), preferred_element_type=F32)

    shape = (CHIPS, LANES)
    row = lax.broadcasted_iota(I32, shape, 0)
    lane = lax.broadcasted_iota(I32, shape, 1)

    lens = lens_ref[...].reshape(CHIPS, 2 * LANES)
    lens = jnp.where(lane < SLOTS, lens[:, :LANES], pltpu.roll(lens[:, LANES:], SLOTS, 1))
    lens = jnp.where(lane < CHIP_SLOTS, (lens + 1) >> 1, 0)
    flat = dest_ref[...]
    turned = pltpu.roll(flat, CHIP_SLOTS, 1)
    to = jnp.concatenate([(turned if c & 1 else flat)[c >> 1:(c >> 1) + 1] for c in range(CHIPS)], axis=0)
    rel = (to >> 6) ^ row
    early = (lens + 1) >> 1
    parts = [early.astype(F32), (lens - early).astype(F32)]

    def top_of(a):
        return jnp.max(jnp.max(a, axis=1, keepdims=True), axis=0, keepdims=True)

    tri = tri_ref[...]
    dmat = dmat_ref[...]
    demand = []
    for beta in range(2):
        mine = [jnp.where(rel == b, parts[beta], 0.0) for b in DESTS]
        earlier = plain(jnp.concatenate(mine, axis=0), tri)
        starts = jnp.zeros(shape, F32)
        total = jnp.zeros(shape, F32)
        for b in DESTS:
            starts = jnp.where(rel == b, earlier[(b - 1) * CHIPS:b * CHIPS], starts)
            total = total + jnp.sum(mine[b - 1], axis=1, keepdims=True) * dmat[b:b + 1]
        demand.append(total)
        at = S_ROW + CHIPS * beta
        out_ref[at:at + CHIPS, :] = starts.astype(I32)

    def flip(a, bit):
        return jnp.where((row & bit) == 0, pltpu.roll(a, CHIPS - bit, 0), pltpu.roll(a, bit, 0))

    def link_loads(x, dot):
        y = dot(x, hop_ref[...])
        for bit in BITS[::-1]:
            y = y + flip(pltpu.roll(y, LANES - PLACE_LANES * bit, 1), bit)
            y = jnp.where(lane < PLACE_LANES * bit, y, 0.0)
        return y

    def path_cost(p):
        y = jnp.where(lane < PLACE_LANES, p, 0.0)
        for bit in BITS:
            y = y + pltpu.roll(flip(y, bit), PLACE_LANES * bit, 1)
        return plain(y, hop_t_ref[...])

    both = demand[0] + demand[1]
    used = jnp.sum(dmat, axis=0, keepdims=True) > 0

    def norm(w):
        w = jnp.where(used, jnp.maximum(w, 1e-6), 0.0)
        return w / jnp.where(used, plain(w, group_ref[...]), 1.0)

    weight = norm(jnp.ones(shape, F32))

    def improve(_, carry):
        weight, best, best_top, drift, size = carry
        loads = link_loads(weight * both, plain)
        top = top_of(loads)
        better = top < best_top
        best = jnp.where(better, weight, best)
        best_top = jnp.where(better, top, best_top)
        price = loads / jnp.maximum(top, 1.0)
        price = price * price
        cost = path_cost(price * price * price)
        drift = MOMENTUM * drift + cost
        weight = norm(weight * jnp.exp(-size * (MOMENTUM * drift + cost)))
        return weight, best, best_top, drift, size * SHRINK

    one = jnp.ones((1, 1), F32)
    start = (weight, weight, 3e38 * one, jnp.zeros(shape, F32), FIRST_STEP * one)
    best = lax.fori_loop(0, ITERS, improve, start)[1]

    best = best / jnp.where(used, exact(best, group_ref[...]), 1.0)
    begins = exact(best, before_ref[...])
    pick = jnp.zeros((1, 1), I32)
    for t in range(2):
        total = demand[t]
        lo = jnp.floor(total * begins)
        x = jnp.where(last_ref[...] > 0, total, pltpu.roll(lo, LANES - 1, 1)) - lo
        top = top_of(link_loads(x, exact))
        top = jnp.where(top_of(-x) > 0.0, 1e6, top)
        need = jnp.zeros((1, 1), I32)
        for rows in CLASSES:
            need = need + (top > caps_of(rows)).astype(I32)
        pick = jnp.maximum(pick, need)
        at = X_ROW + CHIPS * t
        out_ref[at:at + CHIPS, :] = x.astype(I32)
        at = LO_ROW + CHIPS * t
        out_ref[at:at + CHIPS, :] = lo.astype(I32)

    from_dev = 2 * row + (lane >> 5)
    to_dev = to >> 5
    crossing = jnp.where(from_dev == to_dev, 0.0, parts[0])
    come = jnp.concatenate([jnp.where(to_dev == d, crossing, 0.0) for d in range(DEVS)], axis=0)
    come = plain(come, jnp.ones((LANES, LANES), F32)).reshape(DEVS, CHIPS, LANES)
    over = top_of(jnp.sum(come, axis=1)) - POST
    for core in range(2):
        leave = jnp.where((lane >> 5) == core, crossing, 0.0)
        over = jnp.maximum(over, top_of(jnp.sum(leave, axis=1, keepdims=True)) - PRE)
    pick = jnp.where(over > 0.0, len(CLASSES), pick)
    out_ref[C_ROW:C_ROW + CHIPS, :] = jnp.broadcast_to(pick, shape)


def make_plan(lens_all, dest_slot):
    return pl.pallas_call(
        plan_kernel,
        out_shape=jax.ShapeDtypeStruct((META_ROWS, LANES), I32),
        name='plan',
    )(lens_all, dest_slot.reshape(KV, LANES), *plan_consts())


def gather_kernel(x_ref, out_ref, send_sem, recv_sem):
    me = lax.axis_index('dp')
    barrier = pltpu.get_barrier_semaphore()
    for r in range(1, DEVS):
        pl.semaphore_signal(barrier, inc=1, device_id=(lax.rem(me + r, DEVS),), device_id_type=pl.DeviceIdType.MESH)
    pl.semaphore_wait(barrier, DEVS - 1)
    copies = []
    for r in range(1, DEVS):
        copies.append(pltpu.make_async_remote_copy(
            src_ref=x_ref, dst_ref=out_ref.at[me], send_sem=send_sem.at[r], recv_sem=recv_sem.at[r],
            device_id=(lax.rem(me + r, DEVS),), device_id_type=pl.DeviceIdType.MESH))
        copies[-1].start()
    out_ref[me] = x_ref[...]
    for copy in copies:
        copy.wait()


def gather_lens(my_lens):
    row = jnp.pad(my_lens, (0, LANES - SLOTS)).reshape(1, LANES)
    return pl.pallas_call(
        gather_kernel,
        out_shape=jax.ShapeDtypeStruct((DEVS, 1, LANES), I32),
        in_specs=[VMEM], out_specs=VMEM,
        scratch_shapes=[pltpu.SemaphoreType.DMA((DEVS,))] * 2,
        compiler_params=pltpu.CompilerParams(collective_id=0, has_side_effects=True),
        name='gather_lens',
    )(row).reshape(DEVS, LANES)


def length(lens_ref, slot):
    return lens_ref[(slot >> 5) * LANES + (slot & 31)]


def pairs_of(m):
    return (m + 1) >> 1


def part_of(m, beta):
    early = (m + 3) >> 2
    return (0, early)[beta], (early, pairs_of(m) - early)[beta]


def row_copy(src, s0, dst, d0, n, sem):
    return pltpu.make_async_copy(src.at[pl.ds(s0, n)], dst.at[pl.ds(d0, n)], sem)


def drain(ref, n, sem):
    @pl.when(n > 0)
    def _():
        row_copy(ref, 0, ref, 0, n, sem).wait()


def flush(stage, s0, out, n, sem):
    @pl.when(n > 0)
    def _():
        copy = row_copy(stage, s0, out, 0, n, sem)
        copy.start()
        copy.wait()


def start_copy(core, flip, k_ref, v_ref, s0, dst, d0, n, sem):
    for c, ref in enumerate((v_ref, k_ref) if flip else (k_ref, v_ref)):
        @pl.when(core == c)
        def _(ref=ref):
            row_copy(ref, s0, dst, d0, n, sem).start()


SMEM = pl.BlockSpec(memory_space=pltpu.SMEM)
ANY = pl.BlockSpec(memory_space=pltpu.HBM)
VMEM = pl.BlockSpec(memory_space=pltpu.VMEM)


def rows_of(n, dtype=BF):
    return jax.ShapeDtypeStruct((n, TILE, DIM), dtype)


def local_call(kernel, **kwargs):
    return pl.pallas_call(
        kernel, compiler_params=pltpu.CompilerParams(vmem_limit_bytes=VMEM_LIMIT), **kwargs)


def pre_kernel(beta, with_src, dev_ref, lens_ref, dest_ref, k_ref, v_ref, out_ref, *rest):
    if with_src:
        src_ref, stage, sem = rest
    else:
        stage, sem = rest
    dev = dev_ref[0]
    core = dev & 1

    def one(i, q):
        start, n = part_of(lens_ref[i], beta)
        moving = (dest_ref[dev * SLOTS + i] >> 5) != dev
        n = jnp.where(moving, n, 0)

        @pl.when(n > 0)
        def _():
            start_copy(core, True, k_ref, v_ref, i * ROWS + start, stage, q, n, sem)

        return q + n

    total = lax.fori_loop(0, SLOTS, one, I32(0))
    if with_src:
        def invert(i, _):
            for u in range(CHIPS):
                at = i * CHIPS + u
                src_ref[dest_ref[at]] = at
            return 0

        lax.fori_loop(0, TOTAL // CHIPS, invert, 0)
    drain(stage, total, sem)
    flush(stage, 0, out_ref, jnp.minimum(total, PRE), sem)


def pre_pack(beta, with_src, dev, lens, dest, k, v):
    out, specs = [rows_of(PRE)], [ANY]
    if with_src:
        out.append(jax.ShapeDtypeStruct((TOTAL,), I32))
        specs.append(SMEM)
    got = local_call(
        functools.partial(pre_kernel, beta, with_src),
        out_shape=out, out_specs=specs, in_specs=[SMEM] * 3 + [ANY] * 2,
        scratch_shapes=[pltpu.VMEM((SLOTS * HALF, TILE, DIM), BF), pltpu.SemaphoreType.DMA],
    )(dev, lens, dest, k, v)
    return got if with_src else got[0]


class Table:
    def __init__(self, meta, chip, beta):
        self.meta, self.at = meta, CHIPS * BATCHES[beta]
        self.row = [(self.at + (chip ^ v)) * LANES for v in range(CHIPS)]

    def x(self, v, o):
        return self.meta[X_ROW * LANES + self.row[v] + o]

    def lo(self, v, o):
        return self.meta[LO_ROW * LANES + self.row[v] + o]

    def start(self, slot):
        return self.meta[S_ROW * LANES + (self.at + (slot // CHIP_SLOTS)) * LANES + (slot & 63)]


def pack_kernel(beta, step, cap, dev_ref, meta, lens_ref, dest_ref, k_ref, v_ref, pre_ref, *rest):
    recv = {}
    n_in = 3 * step
    for q in range(n_in):
        recv[q // 3, q % 3] = rest[q]
    outs = rest[n_in:n_in + 3]
    stage, table_lo, table_hi, table_to, sem, sem_out = rest[n_in + 3:]
    dev = dev_ref[0]
    chip, core = dev >> 1, dev & 1
    plan = Table(meta, chip, beta)
    used = []
    count = I32(0)
    for k in range(LINKS):
        where = I32(0)
        spans = {}
        for place, o, _ in FLOWS[step, k]:
            if place == 0:
                b = OPTIONS[o][0]
                n = plan.x(0, o)
                if b not in spans:
                    spans[b] = [plan.lo(0, o), I32(0), where]
                spans[b][1] = spans[b][1] + n
                where = where + n
        for b in DESTS:
            if b in spans:
                lo, n, to = spans[b]
                table_lo[b * 3 + k] = lo
                table_hi[b * 3 + k] = lo + n
                table_to[b * 3 + k] = to - lo + k * cap
            else:
                table_lo[b * 3 + k] = I32(0)
                table_hi[b * 3 + k] = I32(0)
                table_to[b * 3 + k] = I32(0)
        used.append(where)
        count = count + where

    if step > 0:
        came = {}
        for (st, kk), runs in FLOWS.items():
            if st < step:
                at = I32(0)
                for place, o, h in runs:
                    v = place ^ (1 << kk)
                    n = plan.x(v, o)
                    hops = OPTIONS[o][1]
                    if h + 1 < len(hops) and hops[h + 1][0] == step:
                        came[v, o] = (st, kk, at, n)
                    at = at + n
        for k in range(LINKS):
            for place, o, h in FLOWS[step, k]:
                if place == 0:
                    continue
                st, kk, at, n = came[place, o]

                @pl.when(n > 0)
                def _(st=st, kk=kk, at=at, n=n, to=used[k], k=k):
                    row_copy(recv[st, kk], at, stage, to + k * cap, n, sem).start()

                used[k] = used[k] + n
                count = count + n

    def one(i, q):
        slot = chip * 64 + i
        to_slot = dest_ref[slot]
        mine = (i >> 5) == core
        start, n = part_of(length(lens_ref, slot), beta)
        b = chip ^ (to_slot >> 6)

        @pl.when(b > 0)
        def _():
            begin = plan.start(slot)
            for k in range(LINKS):
                lo = jnp.maximum(begin, table_lo[b * 3 + k])
                hi = jnp.minimum(begin + n, table_hi[b * 3 + k])
                size = hi - lo
                to = table_to[b * 3 + k] + lo
                skip = lo - begin

                @pl.when(size > 0)
                def _():
                    home = (i & 31) * ROWS + start + skip

                    @pl.when(mine)
                    def _():
                        start_copy(core, False, k_ref, v_ref, home, stage, to, size, sem)

                    @pl.when(jnp.logical_not(mine))
                    def _():
                        row_copy(pre_ref, q + skip, stage, to, size, sem).start()

        away = jnp.logical_not(mine) & ((to_slot >> 5) != (slot >> 5))
        return q + jnp.where(away, n, 0)

    lax.fori_loop(0, 64, one, I32(0))
    drain(stage, count, sem)
    for k in range(LINKS):
        @pl.when(used[k] > 0)
        def _(k=k):
            row_copy(stage, k * cap, outs[k], 0, used[k], sem_out.at[k]).start()
    for k in range(LINKS):
        @pl.when(used[k] > 0)
        def _(k=k):
            row_copy(stage, k * cap, outs[k], 0, used[k], sem_out.at[k]).wait()


def pack(beta, step, cap, scalars, k, v, pre, recv):
    dev, meta, lens, dest, _ = scalars
    recv = [recv[q // 3, q % 3] for q in range(3 * step)]
    return local_call(
        functools.partial(pack_kernel, beta, step, cap),
        out_shape=[rows_of(cap)] * 3, out_specs=[ANY] * 3,
        in_specs=[SMEM] * 4 + [ANY] * (3 + len(recv)),
        scratch_shapes=[pltpu.VMEM((3 * cap, TILE, DIM), BF)] + [pltpu.SMEM((TABLES,), I32)] * 3
        + [pltpu.SemaphoreType.DMA, pltpu.SemaphoreType.DMA((3,))],
    )(dev, meta, lens, dest, k, v, pre, *recv)


def table_kernel(dev_ref, meta, lo_ref, hi_ref, at_ref, buf_ref):
    for beta in BATCHES:
        plan = Table(meta, dev_ref[0] >> 1, beta)
        base = TABLES * beta
        for (st, kk), runs in FLOWS.items():
            at = I32(0)
            for place, o, h in runs:
                v = place ^ (1 << kk)
                n = plan.x(v, o)
                if h + 1 == len(OPTIONS[o][1]):
                    lo = plan.lo(v, o)
                    lo_ref[base + o] = lo
                    hi_ref[base + o] = lo + n
                    at_ref[base + o] = at - lo
                    buf_ref[base + o] = I32(st * 3 + kk)
                at = at + n


def arrivals(dev, meta):
    return local_call(
        table_kernel, out_shape=[jax.ShapeDtypeStruct((2 * TABLES,), I32)] * 4,
        out_specs=[SMEM] * 4, in_specs=[SMEM] * 2)(dev, meta)


def static_lookup(table, index):
    out = I32(table[0])
    for q in range(1, len(table)):
        out = jnp.where(index == q, I32(table[q]), out)
    return out


def from_links(plan, chip, slot, n, tables, base, recv, dst, to, sem):
    table_lo, table_hi, table_at, buf_ref = tables
    b = chip ^ (slot // CHIP_SLOTS)
    begin = plan.start(slot)
    first = static_lookup([0] + OPT_BASE, b)
    count = static_lookup([0] + OPT_COUNT, b)

    def piece(q, _):
        o = first + q
        lo = jnp.maximum(begin, table_lo[base + o])
        hi = jnp.minimum(begin + n, table_hi[base + o])
        size = hi - lo
        at = table_at[base + o] + lo
        put = to + lo - begin

        @pl.when(size > 0)
        def _():
            which = buf_ref[base + o]
            for w in range(9):
                @pl.when(which == w)
                def _(w=w):
                    row_copy(recv[w], at, dst, put, size, sem).start()

        return 0

    lax.fori_loop(0, count, piece, 0)


def post_kernel(beta, other, dev_ref, meta, lens_ref, dest_ref, src_ref, *rest):
    tables, (k_ref, v_ref, pre_ref, *recv), rest = rest[:4], rest[4:16], rest[16:]
    if other:
        out_ref, stage, sem = rest
    else:
        ko_ref, vo_ref, stage, pre_at, sem, sem_out = rest[2:]
    dev = dev_ref[0]
    chip, core = dev >> 1, dev & 1
    plan = Table(meta, chip, beta)
    sibling = dev ^ 1
    target = sibling if other else dev

    if not other:
        def place(i, q):
            pre_at[i] = q
            slot = sibling * SLOTS + i
            _, n = part_of(length(lens_ref, slot), beta)
            return q + jnp.where((dest_ref[slot] >> 5) != sibling, n, 0)

        lax.fori_loop(0, SLOTS, place, I32(0))

    def one(j, q):
        slot = src_ref[target * SLOTS + j]
        start, n = part_of(length(lens_ref, slot), beta)
        owner = slot >> 5
        n = jnp.where(owner == target, 0, n)
        i = slot & 31

        @pl.when(((owner >> 1) == chip) & (n > 0))
        def _():
            if other:
                start_copy(core, False, k_ref, v_ref, i * ROWS + start, stage, q, n, sem)
            else:
                row_copy(pre_ref, pre_at[i], stage, q, n, sem).start()

        @pl.when((owner >> 1) != chip)
        def _():
            from_links(plan, chip, slot, n, tables, TABLES * beta, recv, stage, q, sem)

        return q + n

    total = lax.fori_loop(0, SLOTS, one, I32(0))
    drain(stage, total, sem)
    if other:
        flush(stage, 0, out_ref, total, sem)
        return

    def put(j, q):
        slot = src_ref[target * SLOTS + j]
        start, n = part_of(length(lens_ref, slot), beta)
        n = jnp.where((slot >> 5) == target, 0, n)

        @pl.when(n > 0)
        def _():
            for c, out in enumerate((ko_ref, vo_ref)):
                @pl.when(core == c)
                def _(out=out):
                    row_copy(stage, q, out, j * ROWS + start, n, sem_out).start()

        return q + n

    lax.fori_loop(0, SLOTS, put, I32(0))
    drain(stage, total, sem_out)


def post_pack(beta, scalars, tables, k, v, pre, recv):
    return local_call(
        functools.partial(post_kernel, beta, True),
        out_shape=rows_of(POST), out_specs=ANY,
        in_specs=[SMEM] * 9 + [ANY] * 12,
        scratch_shapes=[pltpu.VMEM((POST, TILE, DIM), BF), pltpu.SemaphoreType.DMA],
    )(*scalars, *tables, k, v, pre, *[recv[q // LINKS, q % LINKS] for q in range(LINKS * LINKS)])


def land(beta, scalars, tables, k, v, pre, recv, outs):
    in_specs = [SMEM] * 9 + [ANY] * 12
    return local_call(
        functools.partial(post_kernel, beta, False),
        out_shape=[rows_of(SLOTS * ROWS)] * 2, out_specs=[ANY] * 2, in_specs=in_specs + [ANY] * 2,
        input_output_aliases={len(in_specs): 0, len(in_specs) + 1: 1},
        scratch_shapes=[pltpu.VMEM((POST, TILE, DIM), BF), pltpu.SMEM((SLOTS,), I32)] + [pltpu.SemaphoreType.DMA] * 2,
    )(*scalars, *tables, k, v, pre, *[recv[q // LINKS, q % LINKS] for q in range(LINKS * LINKS)], *outs)


ZEROS = 256


def zeros_kernel(dev_ref, lens_ref, src_ref, q_ref, ko_ref, vo_ref, lens_out, q_out, zeros, sem):
    dev = dev_ref[0]

    def clear(t, _):
        zeros[pl.ds(t * SLOTS, SLOTS)] = jnp.zeros((SLOTS, TILE, DIM), BF)
        return 0

    lax.fori_loop(0, ZEROS // SLOTS, clear, 0)

    def each(wait, j, _):
        m = length(lens_ref, src_ref[dev * SLOTS + j])
        behind = (m >> 1) + 1
        n = ROWS - behind
        if not wait:
            lens_out[j] = m + 1

        @pl.when(n > 0)
        def _():
            for q, out in enumerate((ko_ref, vo_ref)):
                copy = row_copy(zeros, 0, out, j * ROWS + behind, n, sem.at[q, j])
                copy.wait() if wait else copy.start()

        return 0

    lax.fori_loop(0, SLOTS, functools.partial(each, False), 0)
    q_out[...] = jnp.zeros_like(q_out)
    q_out[:, :HEADS] = q_ref[...]
    lax.fori_loop(0, SLOTS, functools.partial(each, True), 0)


def zero_tails(dev, lens, src, query):
    return local_call(
        zeros_kernel,
        out_shape=[rows_of(SLOTS * ROWS)] * 2 + [jax.ShapeDtypeStruct((SLOTS,), I32),
                                               jax.ShapeDtypeStruct((SLOTS, PADDED, DIM), BF)],
        out_specs=[ANY, ANY, SMEM, VMEM], in_specs=[SMEM] * 3 + [VMEM],
        scratch_shapes=[pltpu.VMEM((ZEROS, TILE, DIM), BF), pltpu.SemaphoreType.DMA((2, SLOTS))],
    )(dev, lens, src, query)


N_BUF, AHEAD, UNROLL = 12, 8, 4


def finish_kernel(dev_ref, lens_ref, src_ref, k_ref, v_ref, *rest):
    post = rest[0:2]
    q_ref, kn_ref, vn_ref, _, _, attn_ref, ko_ref, vo_ref, bufs, cols, moved_at, sem_in, sem_out = rest[2:]
    dev = dev_ref[0]
    core = dev & 1

    def source(j):
        slot = src_ref[dev * SLOTS + j]
        return slot, length(lens_ref, slot)

    def place(j, at):
        slot, m = source(j)
        after = []
        for beta in BATCHES:
            moved_at[SLOTS * beta + j] = at[beta]
            after.append(at[beta] + jnp.where((slot >> 5) != dev, part_of(m, beta)[1], 0))
        return tuple(after)

    lax.fori_loop(0, SLOTS, place, (I32(0), I32(0)))

    def fetch(j):
        slot, m = source(j)
        buf = lax.rem(j, N_BUF)

        @pl.when((slot >> 5) == dev)
        def _():
            home = (slot & 31) * ROWS
            row_copy(k_ref, home, bufs.at[0, buf], 0, pairs_of(m), sem_in.at[0, buf]).start()
            row_copy(v_ref, home, bufs.at[1, buf], 0, pairs_of(m), sem_in.at[1, buf]).start()

        @pl.when((slot >> 5) != dev)
        def _():
            start_copy(core, False, ko_ref, vo_ref, j * ROWS, bufs.at[core, buf], 0, pairs_of(m), sem_in.at[core, buf])
            for beta in BATCHES:
                start, n = part_of(m, beta)
                row_copy(post[beta], moved_at[SLOTS * beta + j], bufs.at[1 - core, buf], start, n,
                         sem_in.at[1 - core, buf]).start()

    def emit(j, wait):
        slot, m = source(j)
        buf = lax.rem(j, N_BUF)
        for q, out in enumerate((ko_ref, vo_ref)):
            here = ((slot >> 5) != dev) & (core == q)
            end = m >> 1
            first = jnp.where(here, end, 0)
            copy = row_copy(bufs.at[q, buf], first, out, j * ROWS + first, end + 1 - first, sem_out.at[q, buf])
            copy.wait() if wait else copy.start()

    def clear(t, _):
        bufs[1, t // 2, pl.ds((t % 2) * DIM, DIM)] = jnp.zeros((DIM, TILE, DIM), BF)
        return 0

    lax.fori_loop(0, 2 * N_BUF, clear, 0)

    def begin(j, _):
        fetch(j)
        return 0

    lax.fori_loop(0, AHEAD, begin, 0)
    half = lax.broadcasted_iota(I32, (TILE, DIM), 0) // KV
    head = lax.broadcasted_iota(I32, (PADDED, LANES), 0) // GROUP
    col = lax.broadcasted_iota(I32, (PADDED, LANES), 1)
    mine = jnp.where(head == (col & (KV - 1)), col, LAST // 2)

    def number(t, _):
        cols[:, pl.ds(pl.multiple_of(t * LANES, LANES), LANES)] = mine + t * LANES
        return 0

    lax.fori_loop(0, TILE * ROWS // LANES, number, 0)

    def some(jj, _):
        def prefetch(u, _):
            ahead = UNROLL * jj + u + AHEAD

            @pl.when(ahead < SLOTS)
            def _():
                @pl.when(ahead >= N_BUF)
                def _():
                    emit(ahead - N_BUF, True)

                fetch(ahead)

            return 0

        lax.fori_loop(0, UNROLL, prefetch, 0)

        def ready(u, _):
            j = UNROLL * jj + u
            _, m = source(j)
            buf = lax.rem(j, N_BUF)
            for q, new in enumerate((kn_ref, vn_ref)):
                row_copy(k_ref, 0, bufs.at[q, buf], 0, pairs_of(m), sem_in.at[q, buf]).wait()
                both = jnp.concatenate([new[j], new[j]], axis=0)
                kept = jnp.where(half < (m & 1), bufs[q, buf, m >> 1], jnp.zeros_like(both))
                bufs[q, buf, m >> 1] = jnp.where(half == (m & 1), both, kept)
            emit(j, False)
            return 0

        lax.fori_loop(0, UNROLL, ready, 0)
        scores = []
        for u in range(UNROLL):
            j = UNROLL * jj + u
            kk = bufs[0, lax.rem(j, N_BUF)].reshape(TILE * ROWS, DIM)
            s = lax.dot_general(q_ref[j], kk, (((1,), (1,)), ((), ())), preferred_element_type=F32)
            scores.append(jnp.where(cols[...] < KV * (source(j)[1] + 1), s * (DIM ** -0.5), -1e30))
        for u, s in enumerate(scores):
            j = UNROLL * jj + u
            p = jnp.exp(s - jnp.max(s, axis=1, keepdims=True))
            total = jnp.sum(p, axis=1, keepdims=True)
            vv = bufs[1, lax.rem(j, N_BUF)].reshape(TILE * ROWS, DIM)
            acc = jnp.dot(p.astype(BF), vv, preferred_element_type=F32)
            attn_ref[j] = (acc / total)[:HEADS].astype(BF)
        return 0

    lax.fori_loop(0, SLOTS // UNROLL, some, 0)

    def wait_out(j, _):
        emit(j, True)
        return 0

    lax.fori_loop(SLOTS - N_BUF, SLOTS, wait_out, 0)


def finish(scalars, k, v, post, query, k_new, v_new, outs):
    in_specs = [SMEM] * 3 + [ANY] * 4 + [VMEM] * 3
    dev, _, lens, _, src = scalars
    attn, ko, vo = local_call(
        finish_kernel,
        out_shape=[jax.ShapeDtypeStruct((SLOTS, HEADS, DIM), BF)] + [rows_of(SLOTS * ROWS)] * 2,
        out_specs=[VMEM, ANY, ANY], in_specs=in_specs + [ANY] * 2,
        input_output_aliases={len(in_specs): 1, len(in_specs) + 1: 2},
        scratch_shapes=[pltpu.VMEM((2, N_BUF, ROWS, TILE, DIM), BF), pltpu.VMEM((PADDED, TILE * ROWS), I32),
                        pltpu.SMEM((2 * SLOTS,), I32)] + [pltpu.SemaphoreType.DMA((2, N_BUF))] * 2,
    )(dev, lens, src, k, v, *post, query, k_new, v_new, *outs)
    return attn, ko, vo


def swap(x, mask):
    return lax.ppermute(x, 'dp', [(i, i ^ mask) for i in range(DEVS)])


def after(x, *others):
    return lax.optimization_barrier((x, *others))[0]


def routed(rows, scalars, k, v, pre0, my_lens, query):
    dev, meta, lens, dest, src = scalars
    cap = caps_of(rows)
    recv, pre = [{}, {}], [pre0, None]
    turn = dev
    for step in range(LINKS):
        for beta in BATCHES:
            if step == 0 and beta == 1:
                pre_send = pre_pack(1, False, turn, my_lens, dest, k, v)
                pre[1] = swap(pre_send, 1)
                ko, vo, lens_out, query = zero_tails(
                    after(dev, pre_send), lens, src, after(query, pre_send).transpose(1, 0, 2))
                tables = arrivals(after(dev, lens_out), meta)
                turn = after(dev, tables[0])
            sends = pack(beta, step, cap, (turn, *scalars[1:]), k, v, pre[beta], recv[beta])
            turn = after(dev, sends[0])
            for dim in range(LINKS):
                recv[beta][step, dim] = swap(sends[dim], 2 << dim)
    post, outs = [], (ko, vo)
    for beta in BATCHES:
        packed = post_pack(beta, (turn, *scalars[1:]), tables, k, v, pre[beta], recv[beta])
        turn = after(dev, packed)
        post.append(swap(packed, 1))
        outs = land(beta, (turn, *scalars[1:]), tables, k, v, pre[beta], recv[beta], outs)
        turn = after(dev, outs[0])
    return *post, *outs, query, lens_out


def take_kernel(owner_ref, dev_ref, src_ref, kh, vh, _, __, ka, va, stage, sem):
    def one(j, _):
        slot = src_ref[dev_ref[0] * SLOTS + j]

        @pl.when((slot >> 5) == owner_ref[0])
        def _():
            for held, out in ((kh, ka), (vh, va)):
                row_copy(held, (slot & 31) * ROWS, stage, 0, ROWS, sem).start()
                row_copy(held, (slot & 31) * ROWS, stage, 0, ROWS, sem).wait()
                row_copy(stage, 0, out, j * ROWS, ROWS, sem).start()
                row_copy(stage, 0, out, j * ROWS, ROWS, sem).wait()

        return 0

    lax.fori_loop(0, SLOTS, one, 0)


def ring_move(dev, src, k, v):
    shift = [(i, (i + 1) % DEVS) for i in range(DEVS)]

    def turn(r, carry):
        owner = (dev - r) % DEVS
        ka, va = local_call(
            take_kernel, out_shape=[rows_of(SLOTS * ROWS)] * 2, out_specs=[ANY] * 2,
            in_specs=[SMEM] * 3 + [ANY] * 4, input_output_aliases={5: 0, 6: 1},
            scratch_shapes=[pltpu.VMEM((ROWS, TILE, DIM), BF), pltpu.SemaphoreType.DMA],
        )(owner, dev, src, *carry)
        return *[lax.ppermute(x, 'dp', shift) for x in carry[:2]], ka, va

    first = turn(0, (k, v, jnp.zeros_like(k), jnp.zeros_like(v)))
    return lax.fori_loop(1, DEVS, turn, first)[2:]


def solution(mesh):
    def local(query, k_cache, v_cache, cache_lens, dest_slot, k_new, v_new):
        dev = lax.axis_index('dp').reshape(1).astype(I32)
        flat, full = (SLOTS * ROWS, TILE, DIM), k_cache.shape
        k, v = k_cache.reshape(flat), v_cache.reshape(flat)
        lens = gather_lens(cache_lens)
        pre_send, src = pre_pack(0, True, after(dev, lens), cache_lens, dest_slot, k, v)
        pre0 = swap(pre_send, 1)
        plan = make_plan(lens, dest_slot)
        scalars = (dev, plan.reshape(-1), lens.reshape(-1), dest_slot, src)

        def route(rows, args):
            return routed(rows, *args)

        def fast(args):
            scalars, k, v, pre0, my_lens, query, k_new, v_new, pick = args
            branches = [functools.partial(route, rows) for rows in CLASSES]
            *post, ko, vo, query, lens_out = lax.switch(pick, branches, (scalars, k, v, pre0, my_lens, query))
            return *finish(scalars, k, v, post, query, k_new, v_new, (ko, vo)), lens_out

        def slow(args):
            (dev, meta, lens, dest, src), k, v, _, _, query, k_new, v_new, _ = args
            ka, va = ring_move(dev, src, k, v)
            mine = length(lens, lax.dynamic_slice(src, (dev[0] * SLOTS,), (SLOTS,)))
            mine = jnp.tile(jnp.pad(mine, (0, LANES - SLOTS)), DEVS)
            here = (dev, meta, mine, dest, jnp.arange(TOTAL, dtype=I32))
            none = [jnp.zeros((CHIPS, TILE, DIM), BF)] * 2
            *outs, lens_out, query = zero_tails(dev, mine, here[-1], after(query, ka).transpose(1, 0, 2))
            return *finish(here, ka, va, none, query, k_new, v_new, outs), lens_out

        pick = plan[C_ROW, 0]
        attn, ko, vo, lens_out = lax.cond(
            pick < len(CLASSES), fast, slow,
            (scalars, k, v, pre0, cache_lens, query.transpose(1, 0, 2), k_new, v_new, pick))
        return attn, ko.reshape(full), vo.reshape(full), lens_out

    row_spec = P('dp')
    return jax.shard_map(local, mesh=mesh, in_specs=(row_spec, row_spec, row_spec, row_spec, P(), row_spec, row_spec), out_specs=(row_spec, row_spec, row_spec, row_spec), check_vma=False)
```
